32 devices in a mesh: tile: 16 (over z, y, x), lev: 2 (over core).
Axes of the slice: x: 2, y: 2, z: 4, core: 2. Of those that a mesh axis runs over, the one named last changes fastest.
Arguments:
- increments: bfloat16 [136, 256, 1024], P('lev', 'tile'), may hold values from -30 to 30
- projection: bfloat16 [80, 136], replicated, may hold values from -0.5 to 0.5
- helmholtz: float32 [80], P('lev'), may hold values from 0.05 to 4
Outputs:
- solution: float32 [80, 256, 1024], P('lev', 'tile')
- residual: float32 [80, 256, 1024], P('lev', 'tile')
The draws below stay inside these ranges and needn't reach their ends.
All inputs are finite; a program needn't handle non-finite values.
Results may differ from the reference program's by a relative error of at most 0.00075.
Values may be sent and summed in bfloat16 or wider, within the bound.
A program may use at most 192 MiB of HBM per device.

```python
import math
import jax
import jax.numpy as jnp
import numpy as np
from jax import lax

LEVELS = 136
MODES = 80
S = 4
BLOCKS = 2
NY = 1024
NX = 256


def lowpass(field):
    for repeat in range(2):
        field = 0.25 * (jnp.roll(field, 1, 1) + 2.0 * field + jnp.roll(field, -1, 1))
        field = 0.25 * (jnp.roll(field, 1, 2) + 2.0 * field + jnp.roll(field, -1, 2))
    return field


def draw_increments(key, part):
    key_base = jax.random.fold_in(key, 11)
    key_one, key_two = jax.random.split(key_base, 2)
    row_frac = (jnp.arange(NX, dtype=jnp.float32) / NX)[None, :, None]
    base = jnp.clip(jax.random.normal(key_one, (LEVELS, NX, NY), jnp.float32), -6.0, 6.0)
    smooth = lowpass(jnp.clip(jax.random.normal(key_two, (LEVELS, NX, NY), jnp.float32), -6.0, 6.0))
    values = base + 10.0 * row_frac * smooth
    return jnp.clip(values, -30.0, 30.0).astype(jnp.bfloat16)


def levels(stream_key, dims, cuts, least, high):
    loudness, own = 1.0, jax.random.fold_in(stream_key, 6)
    for axis_at, blocks in cuts:
        steps = jnp.exp(jax.random.uniform(jax.random.fold_in(own, axis_at), (blocks,), jnp.float32, least / len(cuts), high / len(cuts)))
        loudness = loudness * jnp.repeat(steps, dims[axis_at] // blocks).reshape([-1 if axis == axis_at else 1 for axis in range(len(dims))])
    return loudness


def normal_values(key, extent, deviation, bound, held_as=jnp.bfloat16):
    entries = deviation * jax.random.normal(key, extent, jnp.float32)
    return jnp.clip(entries, min=-bound, max=bound).astype(held_as)


def setup_inputs(seed: int = 0) -> dict:
    streams_of = jax.random.split(jax.random.key(seed), 4)
    increments = draw_increments(jax.random.fold_in(streams_of[3], 71), 0)
    projection = normal_values(streams_of[1], (MODES, LEVELS), LEVELS ** -0.5, 0.5)
    helmholtz = jnp.clip(jnp.exp(math.log(4.0) - 4.3820266 * jax.random.uniform(streams_of[2], (MODES,), jnp.float32) ** levels(streams_of[2], (MODES,), ((0, 2),), -0.2, 0.2)), 0.05, 4.0)
    return dict(increments=increments, projection=projection, helmholtz=helmholtz)


highest = lax.Precision.HIGHEST


def stencil(field, weight):
    padded = jnp.pad(field, 1)
    beside_all = padded[2:, 1:-1] + padded[:-2, 1:-1] + padded[1:-1, 2:] + padded[1:-1, :-2]
    return weight * beside_all


def shift_matrix():
    width = 2 * S + 1
    table = np.zeros((width, width), np.float32)
    for index in range(S):
        table[index + 1, index] = 1.0
    for index in range(S - 1):
        table[S + 2 + index, S + 1 + index] = 1.0
    return jnp.asarray(table, jnp.float32)


def quadratic(gram, left, right):
    return jnp.dot(left, jnp.dot(gram, right, precision=highest), precision=highest)


def solve_mode(inputs):
    rhs, weight = inputs
    width = 2 * S + 1
    shifter = shift_matrix()
    solution = jnp.zeros_like(rhs)
    resid = rhs
    direction = rhs
    for block_index in range(BLOCKS):
        vectors = [direction]
        current = direction
        for power_index in range(S):
            current = stencil(current, weight)
            vectors.append(current)
        vectors.append(resid)
        current = resid
        for power_index in range(S - 1):
            current = stencil(current, weight)
            vectors.append(current)
        basis = jnp.stack(vectors).reshape(width, -1)
        gram = jnp.dot(basis, basis.T, precision=highest)
        p_coef = jnp.zeros((width,), jnp.float32).at[0].set(1.0)
        r_coef = jnp.zeros((width,), jnp.float32).at[S + 1].set(1.0)
        x_coef = jnp.zeros((width,), jnp.float32)
        squares = quadratic(gram, r_coef, r_coef)
        for step_index in range(S):
            moved = p_coef - jnp.dot(shifter, p_coef, precision=highest)
            alpha = squares / quadratic(gram, p_coef, moved)
            x_coef = x_coef + alpha * p_coef
            r_coef = r_coef - alpha * moved
            fresh = quadratic(gram, r_coef, r_coef)
            p_coef = r_coef + (fresh / squares) * p_coef
            squares = fresh
        solution = solution + jnp.dot(x_coef, basis, precision=highest).reshape(rhs.shape)
        resid = jnp.dot(r_coef, basis, precision=highest).reshape(rhs.shape)
        direction = jnp.dot(p_coef, basis, precision=highest).reshape(rhs.shape)
    return solution, resid


def reference(increments, projection, helmholtz):
    flat = increments.reshape(LEVELS, NX * NY)
    modal = jnp.dot(projection, flat, preferred_element_type=jnp.float32).reshape(MODES, NX, NY)
    weights = 1.0 / (4.0 + helmholtz)
    solution, resid = lax.map(solve_mode, (modal, weights))
    return solution, resid
```

```python
import functools

import jax
import jax.numpy as jnp
from jax import lax
from jax.experimental import pallas as pl
from jax.experimental.pallas import tpu as pltpu
from jax.sharding import PartitionSpec as P

STEPS = 8
HALO = STEPS
HALF = HALO // 2
POWER = 13
SUB = 8
LANE = 128
CHUNKS = 4
MESH = pl.DeviceIdType.MESH
f32 = jnp.float32
bf16 = jnp.bfloat16


def stage_groups(count):
    groups = []
    while count > 1:
        size = next(size for size in (16, 4, 2, count) if count % size == 0)
        groups.append(size)
        count //= size
    return groups


def encode(value, scale):
    a = value * scale
    a4 = (a * a) * (a * a)
    return ((a4 * a4) * (a4 * a)).astype(bf16)


def decode(code, scale):
    code = code.astype(f32)
    size = jnp.exp(jnp.log(jnp.maximum(jnp.abs(code), 2.0 ** -126)) * (1.0 / POWER)) * (1.0 / scale)
    return jnp.where(code > 0.0, size, jnp.where(code < 0.0, -size, 0.0))


def add(left, right):
    if left is None:
        return right
    if right is None:
        return left
    return left + right


def coefficients(products, theta):
    count = 2 * STEPS
    moments = list(products[:2])
    for index in range(2, count):
        moments.append(products[index] + products[index] - moments[index % 2])
    half = 0.5 * theta
    one = jnp.ones_like(theta)
    x, r, p = [None] * STEPS, [one], [one]
    r_moments, p_moments = list(moments), list(moments)
    for step in range(STEPS):
        low, high = step, count - 1 - step
        image = {}
        for l in range(low, high):
            if l == 0:
                image[l] = p_moments[0] - theta * p_moments[1]
            else:
                image[l] = p_moments[l] - half * (p_moments[l + 1] + p_moments[l - 1])
        alpha = r_moments[step] / image[step]
        for k in range(step + 1):
            x[k] = add(x[k], alpha * p[k])
        gain = alpha * half
        twice = alpha * theta
        fresh = []
        for k in range(step + 2):
            value = r[k] if k < len(r) else None
            if k < len(p):
                value = value - alpha * p[k] if value is not None else -(alpha * p[k])
            if k == 1:
                value = add(value, twice * p[0])
            elif k > 1:
                value = add(value, gain * p[k - 1])
            if k + 1 < len(p):
                value = value + gain * p[k + 1]
            fresh.append(value)
        r = fresh
        if step == STEPS - 1:
            break
        old = r_moments[step]
        r_moments = [r_moments[l] - alpha * image[l] if l in image else None for l in range(count)]
        beta = (twice if step == 0 else gain) * r_moments[step + 1] / old
        p = [r[k] + beta * p[k] if k < len(p) else r[k] for k in range(step + 2)]
        p_moments = [r_moments[l] + beta * p_moments[l] if l in image else None for l in range(count)]
    return x, r


def kernel(tiles, levs, groups, rows, modes, cells, levels, inc_ref, proj_ref, helm_ref, sol_ref, res_ref,
           x_all, wide, base, powers, out_buf, in_buf, results, thetas, sums, grams,
           local_sem, swap_send, swap_recv, halo_send, halo_recv, gram_send, gram_recv, write_sems):
    tile = lax.axis_index("tile")
    lev = lax.axis_index("lev")
    part = inc_ref.shape[0]
    across = cells // LANE
    parts = modes // SUB
    barrier = pltpu.get_barrier_semaphore()

    stage_peers = []
    stride = 1
    for size in groups:
        digit = lax.rem(lax.div(tile, stride), size)
        start = tile - digit * stride
        stage_peers.append((digit, [start + lax.rem(digit + j, size) * stride for j in range(1, size)]))
        stride *= size

    count = 0
    for j in range(1, levs):
        pl.semaphore_signal(barrier, 1, device_id=(tile, lax.rem(lev + j, levs)), device_id_type=MESH)
        count += 1
    for peer in (lax.rem(tile + 1, tiles), lax.rem(tile + tiles - 1, tiles)):
        pl.semaphore_signal(barrier, 1, device_id=(peer, lev), device_id_type=MESH)
        count += 1
    for digit, peers in stage_peers:
        for peer in peers:
            pl.semaphore_signal(barrier, 1, device_id=(peer, lev), device_id_type=MESH)
            count += 1

    local = pltpu.make_async_copy(inc_ref, x_all.at[0], local_sem)
    local.start()

    chunk = cells // CHUNKS
    with jax.named_scope("barrier"):
        pl.semaphore_wait(barrier, count)

    def swap(j, c):
        cols = pl.ds(c * chunk, chunk)
        return pltpu.make_async_remote_copy(
            src_ref=inc_ref.at[:, cols], dst_ref=x_all.at[levs - j, :, cols], send_sem=swap_send.at[j - 1, c],
            recv_sem=swap_recv.at[j - 1, c], device_id=(tile, lax.rem(lev + j, levs)), device_id_type=MESH)

    for c in range(CHUNKS):
        for j in range(1, levs):
            swap(j, c).start()

    proj = proj_ref[...].astype(f32)
    own = proj[0:modes]
    for j in range(1, levs):
        own = jnp.where(lev == j, proj[j * modes:(j + 1) * modes], own)
    own_levels = levels // levs
    groups_l = [own[:, j * own_levels:(j + 1) * own_levels] for j in range(levs)]
    col_e = lax.broadcasted_iota(jnp.int32, (own_levels, part), 1)
    row_e = lax.broadcasted_iota(jnp.int32, (own_levels, part), 0) * rows
    onehot = jnp.where((col_e >= row_e) & (col_e < row_e + rows), 1.0, 0.0).astype(bf16)
    col_w = lax.rem(lax.broadcasted_iota(jnp.int32, (2 * modes, part), 1), rows)
    second = jnp.where(lax.broadcasted_iota(jnp.int32, (2 * modes, part), 0) >= modes, 1, 0)
    pick = col_w - second

    def widen(position):
        chosen = groups_l[position]
        for j in range(1, levs):
            chosen = jnp.where(lev == j, groups_l[(j + position) % levs], chosen)
        twice = jnp.concatenate([chosen, chosen], axis=0).astype(bf16)
        repeated = jnp.dot(twice, onehot, preferred_element_type=f32)
        for pair in range(rows // 2):
            wide[position, pair * 2 * modes:(pair + 1) * 2 * modes, :] = jnp.where(
                pick == 2 * pair, repeated, 0.0).astype(bf16)

    def project(position, c):
        cols = slice(c * chunk, (c + 1) * chunk)
        got = jnp.dot(wide[position], x_all[position, :, cols], preferred_element_type=f32)
        got = got.reshape(rows, parts, SUB, chunk)
        for g in range(parts):
            value = got[:, g]
            if position:
                value = base[g, HALO:HALO + rows, :, cols] + value
            base[g, HALO:HALO + rows, :, cols] = value

    with jax.named_scope("widen"):
        widen(0)
    with jax.named_scope("own"):
        local.wait()
        for c in range(CHUNKS):
            project(0, c)
    with jax.named_scope("widen"):
        for j in range(1, levs):
            widen(j)

    diag = lax.broadcasted_iota(jnp.int32, (modes, modes), 0) == lax.broadcasted_iota(jnp.int32, (modes, modes), 1)
    helm = jnp.sum(jnp.where(diag, jnp.broadcast_to(helm_ref[...], (modes, modes)), 0.0), axis=1, keepdims=True)
    thetas[...] = jnp.broadcast_to(4.0 / (4.0 + helm), (modes, LANE))
    has = {0: tile < tiles - 1, 1: tile > 0}
    for side in range(2):
        @pl.when(jnp.logical_not(has[side]))
        def _(side=side):
            in_buf[:, side] = jnp.zeros_like(in_buf[:, side])

    scale = 2.0 ** 9.7 / (0.5 * 30.0 * levels)

    def halo_first(side, half):
        if side == 0:
            return half * HALF
        return rows - (half + 1) * HALF

    def halo_copy(g, side, half):
        peer = lax.rem(tile + tiles - 1, tiles) if side == 0 else lax.rem(tile + 1, tiles)
        return pltpu.make_async_remote_copy(
            src_ref=out_buf.at[g, side, half], dst_ref=in_buf.at[g, side, half], send_sem=halo_send.at[g, side, half],
            recv_sem=halo_recv.at[g, side, half], device_id=(peer, lev), device_id_type=MESH)

    sends = {0: tile > 0, 1: tile < tiles - 1}

    def encode_part(g, half, side, cols):
        first = HALO + halo_first(side, half)
        width = cols.stop - cols.start
        out_buf[g, side, half, :, cols] = encode(base[g, first:first + HALF, :, cols].reshape(HALF * SUB, width), scale)

    def send_part(g, half, side):
        @pl.when(sends[side])
        def _():
            halo_copy(g, side, half).start()

    with jax.named_scope("other"):
        for c in range(CHUNKS):
            for j in range(1, levs):
                swap(j, c).wait_recv()
                project(j, c)
            cols = slice(c * chunk, (c + 1) * chunk)
            for half in range(2):
                for side in range(2):
                    encode_part(0, half, side, cols)
    with jax.named_scope("send"):
        for g in range(parts):
            for half in range(2):
                for side in range(2):
                    if g:
                        encode_part(g, half, side, slice(0, cells))
                    send_part(g, half, side)

    lane = lax.broadcasted_iota(jnp.int32, (SUB, LANE), 1)
    first_lane = lane == 0
    last_lane = lane == LANE - 1
    nothing = jnp.zeros((SUB, LANE), f32)

    def beside(tile_row):
        pieces = [tile_row[:, j * LANE:(j + 1) * LANE] for j in range(across)]
        right = [pltpu.roll(piece, 1, 1) for piece in pieces]
        left = [pltpu.roll(piece, LANE - 1, 1) for piece in pieces]
        result = []
        for j in range(across):
            low = jnp.where(first_lane, right[j - 1] if j else nothing, right[j])
            high = jnp.where(last_lane, left[j + 1] if j + 1 < across else nothing, left[j])
            result.append(low + high)
        return jnp.concatenate(result, axis=1)

    def fold(product):
        pieces = [product[:, j * LANE:(j + 1) * LANE] for j in range(across)]
        while len(pieces) > 1:
            pieces = [pieces[i] + pieces[i + 1] if i + 1 < len(pieces) else pieces[i] for i in range(0, len(pieces), 2)]
        return pieces[0]

    inside = jnp.float32(0.5)
    factor = {0: jnp.where(tile > 0, inside, 0.0), 1: jnp.where(tile < tiles - 1, inside, 0.0)}

    def field(g, k):
        return base.at[g] if k == 0 else powers.at[g % 2, k - 1]

    def extend(g, k, ranges):
        src, dst = field(g, k - 1), field(g, k)
        before = field(g, k - 2) if k > 1 else None
        totals = {}
        for low, high in ranges:
            for row in range(low, high):
                at = row + HALO
                here = src[at]
                around = src[at - 1] + src[at + 1] + beside(here)
                if row < 0:
                    gain = factor[0]
                elif row >= rows:
                    gain = factor[1]
                else:
                    gain = 0.5
                if k == 1:
                    gain = gain * 0.5
                fresh = gain * around
                if before is not None:
                    fresh = fresh - before[at]
                dst[at] = fresh
                if 0 <= row < rows:
                    if k == 1:
                        totals[0] = add(totals.get(0), fold(here * here))
                    totals[2 * k - 1] = add(totals.get(2 * k - 1), fold(here * fresh))
                    if k < STEPS:
                        totals[2 * k] = add(totals.get(2 * k), fold(fresh * fresh))
        for slot, value in totals.items():
            sums[slot] = sums[slot] + value

    def interior(g):
        with jax.named_scope("interior"):
            for k in range(1, STEPS):
                if rows - k > k:
                    extend(g, k, [(k, rows - k)])

    def take(g, half):
        with jax.named_scope("take"):
            for side in range(2):
                @pl.when(has[side])
                def _(side=side):
                    halo_copy(g, side, half).wait_recv()
        with jax.named_scope("decode"):
            for side in range(2):
                if side == 0:
                    first = HALO + rows + half * HALF
                else:
                    first = HALO - (half + 1) * HALF
                base[g, first:first + HALF] = decode(in_buf[g, side, half], scale).reshape(HALF, SUB, cells)

    def outer(g, half):
        with jax.named_scope("outer"):
            old, new = half * HALF, (half + 1) * HALF
            for k in range(1, STEPS + 1):
                if rows - k + old >= k - old:
                    extend(g, k, [(k - new, k - old), (rows - k + old, rows - k + new)])
                else:
                    middle = rows // 2
                    extend(g, k, [(k - new, middle), (middle, rows - k + new)])

    products = 2 * STEPS

    def gram_copies(g, stage):
        digit, peers = stage_peers[stage]
        return [pltpu.make_async_remote_copy(
            src_ref=grams.at[g, stage, digit], dst_ref=grams.at[g, stage, digit],
            send_sem=gram_send.at[g, stage, j], recv_sem=gram_recv.at[g, stage, digit],
            device_id=(peer, lev), device_id_type=MESH) for j, peer in enumerate(peers)]

    def gram_start(g, stage, table):
        grams[g, stage, stage_peers[stage][0]] = table
        for copy in gram_copies(g, stage):
            copy.start()

    def gram_finish(g, stage):
        digit, peers = stage_peers[stage]
        size = groups[stage]
        for copy in gram_copies(g, stage):
            copy.wait_send()
        for j in range(1, size):
            sender = lax.rem(digit + j, size)
            pltpu.make_async_remote_copy(
                src_ref=grams.at[g, stage, sender], dst_ref=grams.at[g, stage, sender],
                send_sem=gram_send.at[g, stage, j - 1], recv_sem=gram_recv.at[g, stage, sender],
                device_id=(peers[j - 1], lev), device_id_type=MESH).wait_recv()
        tables = [grams[g, stage, j] for j in range(size)]
        while len(tables) > 1:
            tables = [tables[i] + tables[i + 1] if i + 1 < len(tables) else tables[i] for i in range(0, len(tables), 2)]
        return tables[0]

    def total(g):
        with jax.named_scope("total"):
            lanes = lax.broadcasted_iota(jnp.int32, (SUB, LANE), 1)
            table = jnp.zeros((SUB, LANE), f32)
            for slot in range(products):
                table = jnp.where(lanes == slot, jnp.sum(sums[slot], axis=1, keepdims=True), table)
            sums[...] = jnp.zeros_like(sums)
            gram_start(g, 0, table)

    def finish(g):
        with jax.named_scope("gram"):
            for stage in range(len(groups)):
                table = gram_finish(g, stage)
                if stage + 1 < len(groups):
                    gram_start(g, stage + 1, table)
        with jax.named_scope("coef"):
            columns = [jnp.broadcast_to(table[:, slot:slot + 1], (SUB, LANE)) for slot in range(products)]
            x, r = coefficients(columns, thetas[g * SUB:(g + 1) * SUB])
        with jax.named_scope("combine"):
            for row in range(rows):
                at = row + HALO
                solved, left = [], []
                for j in range(across):
                    cols = slice(j * LANE, (j + 1) * LANE)
                    x_sum = r_sum = None
                    for k in range(STEPS + 1):
                        value = field(g, k)[at, :, cols]
                        r_sum = add(r_sum, r[k] * value)
                        if k < STEPS:
                            x_sum = add(x_sum, x[k] * value)
                    solved.append(x_sum)
                    left.append(r_sum)
                results[g, 0, :, row, :] = jnp.concatenate(solved, axis=1)
                results[g, 1, :, row, :] = jnp.concatenate(left, axis=1)
        for out, ref in enumerate((sol_ref, res_ref)):
            pltpu.make_async_copy(results.at[g, out], ref.at[pl.ds(g * SUB, SUB)], write_sems.at[g, out]).start()

    sums[...] = jnp.zeros_like(sums)
    for g in range(parts):
        interior(g)
        if g:
            finish(g - 1)
        for half in range(2):
            take(g, half)
            outer(g, half)
        total(g)
    finish(parts - 1)

    with jax.named_scope("drain"):
        for j in range(1, levs):
            for c in range(CHUNKS):
                swap(j, c).wait_send()
        for g in range(parts):
            for half in range(2):
                for side in range(2):
                    @pl.when(sends[side])
                    def _(g=g, side=side, half=half):
                        halo_copy(g, side, half).wait_send()
        for g in range(parts):
            for out, ref in enumerate((sol_ref, res_ref)):
                pltpu.make_async_copy(results.at[g, out], ref.at[pl.ds(g * SUB, SUB)], write_sems.at[g, out]).wait()


def shards(increments, projection, helmholtz):
    tiles, levs = lax.axis_size("tile"), lax.axis_size("lev")
    own_levels, rows, cells = increments.shape
    modes = projection.shape[0] // levs
    levels = own_levels * levs
    groups = stage_groups(tiles)
    most = max(groups)
    parts = modes // SUB
    vmem = pltpu.VMEM
    dma = pltpu.SemaphoreType.DMA
    scratch = [
        vmem((levs, own_levels * rows, cells), bf16),
        vmem((levs, rows * modes, own_levels * rows), bf16),
        vmem((parts, rows + 2 * HALO, SUB, cells), f32),
        vmem((2, STEPS, rows + 2 * HALO, SUB, cells), f32),
        vmem((parts, 2, 2, HALF * SUB, cells), bf16),
        vmem((parts, 2, 2, HALF * SUB, cells), bf16),
        vmem((parts, 2, SUB, rows, cells), f32),
        vmem((modes, LANE), f32),
        vmem((2 * STEPS, SUB, LANE), f32),
        vmem((parts, len(groups), most, SUB, LANE), f32),
        dma,
        dma((levs - 1, CHUNKS)),
        dma((levs - 1, CHUNKS)),
        dma((parts, 2, 2)),
        dma((parts, 2, 2)),
        dma((parts, len(groups), most)),
        dma((parts, len(groups), most)),
        dma((parts, 2)),
    ]
    shape = jax.ShapeDtypeStruct((modes, rows, cells), f32)
    return pl.pallas_call(
        functools.partial(kernel, tiles, levs, groups, rows, modes, cells, levels),
        out_shape=(shape, shape),
        in_specs=[pl.BlockSpec(memory_space=pl.ANY), pl.BlockSpec(memory_space=pltpu.VMEM),
                  pl.BlockSpec(memory_space=pltpu.VMEM)],
        out_specs=(pl.BlockSpec(memory_space=pl.ANY), pl.BlockSpec(memory_space=pl.ANY)),
        scratch_shapes=scratch,
        compiler_params=pltpu.CompilerParams(collective_id=0, has_side_effects=True, vmem_limit_bytes=67000000),
    )(increments.reshape(own_levels * rows, cells), projection, helmholtz.reshape(1, modes))


def solution(mesh):
    in_specs = (P("lev", "tile", None), P(), P("lev"))
    out_specs = (P("lev", "tile", None), P("lev", "tile", None))
    return jax.shard_map(shards, mesh=mesh, in_specs=in_specs, out_specs=out_specs, check_vma=False)
```

```python
import functools

import jax
import jax.numpy as jnp
from jax import lax
from jax.experimental import pallas as pl
from jax.experimental.pallas import tpu as pltpu
from jax.sharding import PartitionSpec as P

STEPS = 8
HALO = STEPS
HALF = HALO // 2
POWER = 13
SUB = 8
RING = 3
LAG = 2
LANE = 128
CHUNKS = 4
MESH = pl.DeviceIdType.MESH
f32 = jnp.float32
bf16 = jnp.bfloat16


def stage_groups(count):
    groups = []
    while count > 1:
        size = next(size for size in (16, 4, 2, count) if count % size == 0)
        groups.append(size)
        count //= size
    return groups


def encode(value, scale):
    a = value * scale
    a4 = (a * a) * (a * a)
    return ((a4 * a4) * (a4 * a)).astype(bf16)


def decode(code, scale):
    code = code.astype(f32)
    size = jnp.exp(jnp.log(jnp.maximum(jnp.abs(code), 2.0 ** -126)) * (1.0 / POWER)) * (1.0 / scale)
    return jnp.where(code > 0.0, size, jnp.where(code < 0.0, -size, 0.0))


def add(left, right):
    if left is None:
        return right
    if right is None:
        return left
    return left + right


def coefficients(products, theta):
    count = 2 * STEPS
    moments = list(products[:2])
    for index in range(2, count):
        moments.append(products[index] + products[index] - moments[index % 2])
    half = 0.5 * theta
    one = jnp.ones_like(theta)
    x, r, p = [None] * STEPS, [one], [one]
    r_moments, p_moments = list(moments), list(moments)
    for step in range(STEPS):
        low, high = step, count - 1 - step
        image = {}
        for l in range(low, high):
            if l == 0:
                image[l] = p_moments[0] - theta * p_moments[1]
            else:
                image[l] = p_moments[l] - half * (p_moments[l + 1] + p_moments[l - 1])
        alpha = r_moments[step] / image[step]
        for k in range(step + 1):
            x[k] = add(x[k], alpha * p[k])
        gain = alpha * half
        twice = alpha * theta
        fresh = []
        for k in range(step + 2):
            value = r[k] if k < len(r) else None
            if k < len(p):
                value = value - alpha * p[k] if value is not None else -(alpha * p[k])
            if k == 1:
                value = add(value, twice * p[0])
            elif k > 1:
                value = add(value, gain * p[k - 1])
            if k + 1 < len(p):
                value = value + gain * p[k + 1]
            fresh.append(value)
        r = fresh
        if step == STEPS - 1:
            break
        old = r_moments[step]
        r_moments = [r_moments[l] - alpha * image[l] if l in image else None for l in range(count)]
        beta = (twice if step == 0 else gain) * r_moments[step + 1] / old
        p = [r[k] + beta * p[k] if k < len(p) else r[k] for k in range(step + 2)]
        p_moments = [r_moments[l] + beta * p_moments[l] if l in image else None for l in range(count)]
    return x, r


def kernel(tiles, levs, groups, rows, modes, cells, levels, inc_ref, proj_ref, helm_ref, sol_ref, res_ref,
           x_all, wide, base, powers, out_buf, in_buf, thetas, sums, grams,
           local_sem, swap_send, swap_recv, halo_send, halo_recv, gram_send, gram_recv):
    tile = lax.axis_index("tile")
    lev = lax.axis_index("lev")
    part = inc_ref.shape[0]
    across = cells // LANE
    parts = modes // SUB
    barrier = pltpu.get_barrier_semaphore()

    stage_peers = []
    stride = 1
    for size in groups:
        digit = lax.rem(lax.div(tile, stride), size)
        start = tile - digit * stride
        stage_peers.append((digit, [start + lax.rem(digit + j, size) * stride for j in range(1, size)]))
        stride *= size

    count = 0
    for j in range(1, levs):
        pl.semaphore_signal(barrier, 1, device_id=(tile, lax.rem(lev + j, levs)), device_id_type=MESH)
        count += 1
    for peer in (lax.rem(tile + 1, tiles), lax.rem(tile + tiles - 1, tiles)):
        pl.semaphore_signal(barrier, 1, device_id=(peer, lev), device_id_type=MESH)
        count += 1
    for digit, peers in stage_peers:
        for peer in peers:
            pl.semaphore_signal(barrier, 1, device_id=(peer, lev), device_id_type=MESH)
            count += 1

    local = pltpu.make_async_copy(inc_ref, x_all.at[0], local_sem)
    local.start()

    chunk = cells // CHUNKS
    with jax.named_scope("barrier"):
        pl.semaphore_wait(barrier, count)

    def swap(j, c):
        cols = pl.ds(c * chunk, chunk)
        return pltpu.make_async_remote_copy(
            src_ref=inc_ref.at[:, cols], dst_ref=x_all.at[levs - j, :, cols], send_sem=swap_send.at[j - 1, c],
            recv_sem=swap_recv.at[j - 1, c], device_id=(tile, lax.rem(lev + j, levs)), device_id_type=MESH)

    for c in range(CHUNKS):
        for j in range(1, levs):
            swap(j, c).start()

    proj = proj_ref[...].astype(f32)
    own = proj[:, 0:modes]
    for j in range(1, levs):
        own = jnp.where(lev == j, proj[:, j * modes:(j + 1) * modes], own)
    own_levels = levels // levs
    groups_l = [own[j * own_levels:(j + 1) * own_levels] for j in range(levs)]
    col_e = lax.broadcasted_iota(jnp.int32, (own_levels, part), 1)
    row_e = lax.broadcasted_iota(jnp.int32, (own_levels, part), 0) * rows
    onehot = jnp.where((col_e >= row_e) & (col_e < row_e + rows), 1.0, 0.0).astype(bf16)
    col_w = lax.rem(lax.broadcasted_iota(jnp.int32, (2 * modes, part), 1), rows)
    second = jnp.where(lax.broadcasted_iota(jnp.int32, (2 * modes, part), 0) >= modes, 1, 0)
    pick = col_w - second

    def widen(position):
        chosen = groups_l[position]
        for j in range(1, levs):
            chosen = jnp.where(lev == j, groups_l[(j + position) % levs], chosen)
        twice = jnp.concatenate([chosen, chosen], axis=1).astype(bf16)
        repeated = lax.dot_general(twice, onehot, (((0,), (0,)), ((), ())), preferred_element_type=f32)
        for pair in range(rows // 2):
            wide[position, pair * 2 * modes:(pair + 1) * 2 * modes, :] = jnp.where(
                pick == 2 * pair, repeated, 0.0).astype(bf16)

    def project(position, c):
        cols = slice(c * chunk, (c + 1) * chunk)
        got = jnp.dot(wide[position], x_all[position, :, cols], preferred_element_type=f32)
        got = got.reshape(rows, parts, SUB, chunk)
        for g in range(parts):
            value = got[:, g]
            if position:
                value = base[g, HALO:HALO + rows, :, cols] + value
            base[g, HALO:HALO + rows, :, cols] = value

    with jax.named_scope("widen"):
        widen(0)
    with jax.named_scope("own"):
        local.wait()
        for c in range(CHUNKS):
            project(0, c)
    with jax.named_scope("widen"):
        for j in range(1, levs):
            widen(j)

    diag = lax.broadcasted_iota(jnp.int32, (modes, modes), 0) == lax.broadcasted_iota(jnp.int32, (modes, modes), 1)
    helm = jnp.sum(jnp.where(diag, jnp.broadcast_to(helm_ref[...], (modes, modes)), 0.0), axis=1, keepdims=True)
    thetas[...] = jnp.broadcast_to(4.0 / (4.0 + helm), (modes, LANE))
    has = {0: tile < tiles - 1, 1: tile > 0}
    for side in range(2):
        @pl.when(jnp.logical_not(has[side]))
        def _(side=side):
            in_buf[:, side] = jnp.zeros_like(in_buf[:, side])

    scale = 2.0 ** 9.7 / (0.5 * 30.0 * levels)

    def halo_first(side, half):
        if side == 0:
            return half * HALF
        return rows - (half + 1) * HALF

    def halo_copy(g, side, half, cols=slice(None)):
        peer = lax.rem(tile + tiles - 1, tiles) if side == 0 else lax.rem(tile + 1, tiles)
        return pltpu.make_async_remote_copy(
            src_ref=out_buf.at[g, side, half, :, cols], dst_ref=in_buf.at[g, side, half, :, cols], send_sem=halo_send.at[g, side, half],
            recv_sem=halo_recv.at[g, side, half], device_id=(peer, lev), device_id_type=MESH)

    sends = {0: tile > 0, 1: tile < tiles - 1}

    def encode_part(g, half, side, cols):
        first = HALO + halo_first(side, half)
        width = cols.stop - cols.start
        out_buf[g, side, half, :, cols] = encode(base[g, first:first + HALF, :, cols].reshape(HALF * SUB, width), scale)

    def send_chunk(c):
        cols = pl.ds(c * chunk, chunk)
        for half in range(2):
            for side in range(2):
                encode_part(0, half, side, slice(c * chunk, (c + 1) * chunk))

                @pl.when(sends[side])
                def _(half=half, side=side):
                    halo_copy(0, side, half, cols).start()

    def send(g):
        with jax.named_scope("send"):
            for half in range(2):
                for side in range(2):
                    encode_part(g, half, side, slice(0, cells))

                    @pl.when(sends[side])
                    def _(half=half, side=side):
                        halo_copy(g, side, half).start()

    with jax.named_scope("other"):
        for c in range(CHUNKS):
            for j in range(1, levs):
                swap(j, c).wait_recv()
                project(j, c)
            send_chunk(c)
    if parts > 1:
        send(1)

    lane = lax.broadcasted_iota(jnp.int32, (SUB, LANE), 1)
    first_lane = lane == 0
    last_lane = lane == LANE - 1
    nothing = jnp.zeros((SUB, LANE), f32)

    def beside(tile_row):
        pieces = [tile_row[:, j * LANE:(j + 1) * LANE] for j in range(across)]
        right = [pltpu.roll(piece, 1, 1) for piece in pieces]
        left = [pltpu.roll(piece, LANE - 1, 1) for piece in pieces]
        result = []
        for j in range(across):
            low = jnp.where(first_lane, right[j - 1] if j else nothing, right[j])
            high = jnp.where(last_lane, left[j + 1] if j + 1 < across else nothing, left[j])
            result.append(low + high)
        return jnp.concatenate(result, axis=1)

    def fold(product):
        pieces = [product[:, j * LANE:(j + 1) * LANE] for j in range(across)]
        while len(pieces) > 1:
            pieces = [pieces[i] + pieces[i + 1] if i + 1 < len(pieces) else pieces[i] for i in range(0, len(pieces), 2)]
        return pieces[0]

    inside = jnp.float32(0.5)
    factor = {0: jnp.where(tile > 0, inside, 0.0), 1: jnp.where(tile < tiles - 1, inside, 0.0)}

    def field(g, k):
        return base.at[g] if k == 0 else powers.at[lax.rem(g, RING), k - 1]

    def extend(g, k, ranges):
        src, dst = field(g, k - 1), field(g, k)
        before = field(g, k - 2) if k > 1 else None
        totals = {}
        for low, high in ranges:
            for row in range(low, high):
                at = row + HALO
                here = src[at]
                around = src[at - 1] + src[at + 1] + beside(here)
                if row < 0:
                    gain = factor[0]
                elif row >= rows:
                    gain = factor[1]
                else:
                    gain = 0.5
                if k == 1:
                    gain = gain * 0.5
                fresh = gain * around
                if before is not None:
                    fresh = fresh - before[at]
                dst[at] = fresh
                if 0 <= row < rows:
                    if k == 1:
                        totals[0] = add(totals.get(0), fold(here * here))
                    totals[2 * k - 1] = add(totals.get(2 * k - 1), fold(here * fresh))
                    if k < STEPS:
                        totals[2 * k] = add(totals.get(2 * k), fold(fresh * fresh))
        for slot, value in totals.items():
            sums[slot] = sums[slot] + value

    def interior(g):
        with jax.named_scope("interior"):
            for k in range(1, STEPS):
                if rows - k > k:
                    extend(g, k, [(k, rows - k)])

    def take(g, half):
        with jax.named_scope("take"):
            for side in range(2):
                @pl.when(has[side])
                def _(side=side):
                    halo_copy(g, side, half).wait_recv()
        with jax.named_scope("decode"):
            for side in range(2):
                if side == 0:
                    first = HALO + rows + half * HALF
                else:
                    first = HALO - (half + 1) * HALF
                base[g, first:first + HALF] = decode(in_buf[g, side, half], scale).reshape(HALF, SUB, cells)

    def outer(g, half):
        with jax.named_scope("outer"):
            old, new = half * HALF, (half + 1) * HALF
            for k in range(1, STEPS + 1):
                extend(g, k, [(k - new, k - old), (rows - k + old, rows - k + new)])

    products = 2 * STEPS

    def modes_of(g):
        return pl.ds(pl.multiple_of(g * SUB, SUB), SUB)

    def gram_start(g, stage, table):
        digit, peers = stage_peers[stage]
        grams[g, stage, digit] = table
        for peer in peers:
            pltpu.make_async_remote_copy(
                src_ref=grams.at[g, stage, digit], dst_ref=grams.at[g, stage, digit], send_sem=gram_send.at[g, stage],
                recv_sem=gram_recv.at[g, stage], device_id=(peer, lev), device_id_type=MESH).start()

    def gram_finish(g, stage):
        digit, peers = stage_peers[stage]
        size = groups[stage]
        others = grams.at[g, stage, pl.ds(0, size - 1)]
        pltpu.make_async_remote_copy(
            src_ref=others, dst_ref=others, send_sem=gram_send.at[g, stage],
            recv_sem=gram_recv.at[g, stage], device_id=(peers[0], lev), device_id_type=MESH).wait()
        tables = [grams[g, stage, j] for j in range(size)]
        while len(tables) > 1:
            tables = [tables[i] + tables[i + 1] if i + 1 < len(tables) else tables[i] for i in range(0, len(tables), 2)]
        return tables[0]

    def total(g):
        with jax.named_scope("total"):
            lanes = lax.broadcasted_iota(jnp.int32, (SUB, LANE), 1)
            table = jnp.zeros((SUB, LANE), f32)
            for slot in range(products):
                table = jnp.where(lanes == slot, jnp.sum(sums[slot], axis=1, keepdims=True), table)
            sums[...] = jnp.zeros_like(sums)
            gram_start(g, 0, table)

    def finish(g):
        with jax.named_scope("gram"):
            for stage in range(len(groups)):
                table = gram_finish(g, stage)
                if stage + 1 < len(groups):
                    gram_start(g, stage + 1, table)
        with jax.named_scope("coef"):
            columns = [jnp.broadcast_to(table[:, slot:slot + 1], (SUB, LANE)) for slot in range(products)]
            x, r = coefficients(columns, thetas[modes_of(g)])
        with jax.named_scope("combine"):
            for row in range(rows):
                at = row + HALO
                solved, left = [], []
                for j in range(across):
                    cols = slice(j * LANE, (j + 1) * LANE)
                    x_sum = r_sum = None
                    for k in range(STEPS + 1):
                        value = field(g, k)[at, :, cols]
                        r_sum = add(r_sum, r[k] * value)
                        if k < STEPS:
                            x_sum = add(x_sum, x[k] * value)
                    solved.append(x_sum)
                    left.append(r_sum)
                sol_ref[modes_of(g), row, :] = jnp.concatenate(solved, axis=1)
                res_ref[modes_of(g), row, :] = jnp.concatenate(left, axis=1)

    sums[...] = jnp.zeros_like(sums)

    def advance(index, carry):
        @pl.when(index < parts)
        def _():
            interior(index)
            for half in range(2):
                take(index, half)
                outer(index, half)
            total(index)

        @pl.when(index + LAG < parts)
        def _():
            send(index + LAG)

        @pl.when(index >= LAG)
        def _():
            finish(index - LAG)

        return carry

    lax.fori_loop(0, parts + LAG, advance, 0)

    with jax.named_scope("drain"):
        for j in range(1, levs):
            for c in range(CHUNKS):
                swap(j, c).wait_send()
        for g in range(parts):
            for half in range(2):
                for side in range(2):
                    @pl.when(sends[side])
                    def _(g=g, side=side, half=half):
                        halo_copy(g, side, half).wait_send()


def shards(increments, projection, helmholtz):
    tiles, levs = lax.axis_size("tile"), lax.axis_size("lev")
    own_levels, rows, cells = increments.shape
    modes = projection.shape[0] // levs
    levels = own_levels * levs
    groups = stage_groups(tiles)
    most = max(groups)
    parts = modes // SUB
    vmem = pltpu.VMEM
    dma = pltpu.SemaphoreType.DMA
    scratch = [
        vmem((levs, own_levels * rows, cells), bf16),
        vmem((levs, rows * modes, own_levels * rows), bf16),
        vmem((parts, rows + 2 * HALO, SUB, cells), f32),
        vmem((RING, STEPS, rows + 2 * HALO, SUB, cells), f32),
        vmem((parts, 2, 2, HALF * SUB, cells), bf16),
        vmem((parts, 2, 2, HALF * SUB, cells), bf16),
        vmem((modes, LANE), f32),
        vmem((2 * STEPS, SUB, LANE), f32),
        vmem((parts, len(groups), most, SUB, LANE), f32),
        dma,
        dma((levs - 1, CHUNKS)),
        dma((levs - 1, CHUNKS)),
        dma((parts, 2, 2)),
        dma((parts, 2, 2)),
        dma((parts, len(groups))),
        dma((parts, len(groups))),
    ]
    shape = pltpu.VMEM((modes, rows, cells), f32)
    return pl.pallas_call(
        functools.partial(kernel, tiles, levs, groups, rows, modes, cells, levels),
        out_shape=(shape, shape),
        in_specs=[pl.BlockSpec(memory_space=pl.ANY), pl.BlockSpec(memory_space=pltpu.VMEM),
                  pl.BlockSpec(memory_space=pltpu.VMEM)],
        out_specs=(pl.BlockSpec(memory_space=pltpu.VMEM), pl.BlockSpec(memory_space=pltpu.VMEM)),
        scratch_shapes=scratch,
        compiler_params=pltpu.CompilerParams(collective_id=0, has_side_effects=True, vmem_limit_bytes=52000000),
    )(increments.reshape(own_levels * rows, cells), projection.T, helmholtz.reshape(1, modes))


def solution(mesh):
    in_specs = (P("lev", "tile", None), P(), P("lev"))
    out_specs = (P("lev", "tile", None), P("lev", "tile", None))
    return jax.shard_map(shards, mesh=mesh, in_specs=in_specs, out_specs=out_specs, check_vma=False)
```

```python
import functools

import jax
import jax.numpy as jnp
from jax import lax
from jax.experimental import pallas as pl
from jax.experimental.pallas import tpu as pltpu
from jax.sharding import PartitionSpec as P

STEPS = 8
HALO = STEPS
HALF = HALO // 2
POWER = 13
SUB = 8
LANE = 128
CHUNKS = 4
MESH = pl.DeviceIdType.MESH
f32 = jnp.float32
bf16 = jnp.bfloat16


def stage_groups(count):
    groups = []
    while count > 1:
        size = next(size for size in (16, 4, 2, count) if count % size == 0)
        groups.append(size)
        count //= size
    return groups


def reaches(tiles):
    return [2 ** r for r in range(tiles.bit_length()) if 2 ** r < tiles - 1]


def starts(rows):
    places = [0]
    for k in range(1, STEPS + 1):
        places.append(places[-1] + rows + 2 * (HALO - k))
    return places


def encode(value, scale):
    a = value * scale
    a4 = (a * a) * (a * a)
    return ((a4 * a4) * (a4 * a)).astype(bf16)


def decode(code, scale):
    code = code.astype(f32)
    size = jnp.exp(jnp.log(jnp.maximum(jnp.abs(code), 2.0 ** -126)) * (1.0 / POWER)) * (1.0 / scale)
    return jnp.where(code > 0.0, size, jnp.where(code < 0.0, -size, 0.0))


def add(left, right):
    if left is None:
        return right
    if right is None:
        return left
    return left + right


def coefficients(products, theta):
    count = 2 * STEPS
    moments = list(products[:2])
    for index in range(2, count):
        moments.append(products[index] + products[index] - moments[index % 2])
    half = 0.5 * theta
    one = jnp.ones_like(theta)
    x, r, p = [None] * STEPS, [one], [one]
    r_moments, p_moments = list(moments), list(moments)
    for step in range(STEPS):
        low, high = step, count - 1 - step
        image = {}
        for l in range(low, high):
            if l == 0:
                image[l] = p_moments[0] - theta * p_moments[1]
            else:
                image[l] = p_moments[l] - half * (p_moments[l + 1] + p_moments[l - 1])
        alpha = r_moments[step] / image[step]
        for k in range(step + 1):
            x[k] = add(x[k], alpha * p[k])
        gain = alpha * half
        twice = alpha * theta
        fresh = []
        for k in range(step + 2):
            value = r[k] if k < len(r) else None
            if k < len(p):
                value = value - alpha * p[k] if value is not None else -(alpha * p[k])
            if k == 1:
                value = add(value, twice * p[0])
            elif k > 1:
                value = add(value, gain * p[k - 1])
            if k + 1 < len(p):
                value = value + gain * p[k + 1]
            fresh.append(value)
        r = fresh
        if step == STEPS - 1:
            break
        old = r_moments[step]
        r_moments = [r_moments[l] - alpha * image[l] if l in image else None for l in range(count)]
        beta = (twice if step == 0 else gain) * r_moments[step + 1] / old
        p = [r[k] + beta * p[k] if k < len(p) else r[k] for k in range(step + 2)]
        p_moments = [r_moments[l] + beta * p_moments[l] if l in image else None for l in range(count)]
    return x, r


def kernel(tiles, levs, groups, rows, modes, cells, levels, inc_ref, proj_ref, helm_ref, sol_ref, res_ref,
           x_all, wide, base, powers, out_buf, in_buf, thetas, sums, grams, proj_own, helm_own,
           local_sem, small_sems, known, swap_send, swap_recv, halo_send, halo_recv, gram_send, gram_recv):
    tile = lax.axis_index("tile")
    lev = lax.axis_index("lev")
    part = inc_ref.shape[0]
    across = cells // LANE
    parts = modes // SUB
    barrier = pltpu.get_barrier_semaphore()

    stage_peers = []
    stride = 1
    for size in groups:
        digit = lax.rem(lax.div(tile, stride), size)
        start = tile - digit * stride
        stage_peers.append((digit, [start + lax.rem(digit + j, size) * stride for j in range(1, size)]))
        stride *= size

    count = 0
    for j in range(1, levs):
        pl.semaphore_signal(barrier, 1, device_id=(tile, lax.rem(lev + j, levs)), device_id_type=MESH)
        count += 1
    def toward(distance):
        return [(lax.max(tile - distance, 0), tile >= distance),
                (lax.min(tile + distance, tiles - 1), tile < tiles - distance)]

    for peer, there in toward(1):
        @pl.when(there)
        def _(peer=peer):
            pl.semaphore_signal(barrier, 1, device_id=(peer, lev), device_id_type=MESH)
        count += jnp.where(there, 1, 0)
    local = pltpu.make_async_copy(inc_ref, x_all.at[0], local_sem)
    small = [pltpu.make_async_copy(proj_ref, proj_own, small_sems.at[0]),
             pltpu.make_async_copy(helm_ref, helm_own, small_sems.at[1])]
    for copy in small:
        copy.start()
    local.start()

    chunk = cells // CHUNKS
    with jax.named_scope("barrier"):
        pl.semaphore_wait(barrier, count)

    rounds = reaches(tiles)

    def greet(r):
        if r < len(rounds):
            for way, (peer, there) in enumerate(toward(rounds[r])):
                @pl.when(there)
                def _(way=way, peer=peer):
                    pl.semaphore_signal(known.at[r, way], 1, device_id=(peer, lev), device_id_type=MESH)

    def greeted(r):
        if r < len(rounds):
            for way, (peer, there) in enumerate(toward(rounds[r])):
                @pl.when(there)
                def _(way=way):
                    pl.semaphore_wait(known.at[r, 1 - way], 1)

    greet(0)

    def swap(j, c):
        cols = pl.ds(c * chunk, chunk)
        return pltpu.make_async_remote_copy(
            src_ref=inc_ref.at[:, cols], dst_ref=x_all.at[levs - j, :, cols], send_sem=swap_send.at[j - 1, c],
            recv_sem=swap_recv.at[j - 1, c], device_id=(tile, lax.rem(lev + j, levs)), device_id_type=MESH)

    for c in range(CHUNKS):
        for j in range(1, levs):
            swap(j, c).start()

    for copy in small:
        copy.wait()
    proj = proj_own[...].astype(f32)
    own = proj[:, 0:modes]
    for j in range(1, levs):
        own = jnp.where(lev == j, proj[:, j * modes:(j + 1) * modes], own)
    own_levels = levels // levs
    groups_l = [own[j * own_levels:(j + 1) * own_levels] for j in range(levs)]
    col_e = lax.broadcasted_iota(jnp.int32, (own_levels, part), 1)
    row_e = lax.broadcasted_iota(jnp.int32, (own_levels, part), 0) * rows
    onehot = jnp.where((col_e >= row_e) & (col_e < row_e + rows), 1.0, 0.0).astype(bf16)
    col_w = lax.rem(lax.broadcasted_iota(jnp.int32, (2 * modes, part), 1), rows)
    second = jnp.where(lax.broadcasted_iota(jnp.int32, (2 * modes, part), 0) >= modes, 1, 0)
    pick = col_w - second

    def widen(position):
        chosen = groups_l[position]
        for j in range(1, levs):
            chosen = jnp.where(lev == j, groups_l[(j + position) % levs], chosen)
        twice = jnp.concatenate([chosen, chosen], axis=1).astype(bf16)
        repeated = lax.dot_general(twice, onehot, (((0,), (0,)), ((), ())), preferred_element_type=f32)
        for pair in range(rows // 2):
            wide[position, pair * 2 * modes:(pair + 1) * 2 * modes, :] = jnp.where(
                pick == 2 * pair, repeated, 0.0).astype(bf16)

    def project(position, c):
        cols = slice(c * chunk, (c + 1) * chunk)
        got = jnp.dot(wide[position], x_all[position, :, cols], preferred_element_type=f32)
        got = got.reshape(rows, parts, SUB, chunk)
        for g in range(parts):
            value = got[:, g]
            if position:
                value = base[g, HALO:HALO + rows, :, cols] + value
            base[g, HALO:HALO + rows, :, cols] = value

    with jax.named_scope("widen"):
        widen(0)
    with jax.named_scope("own"):
        local.wait()
        for c in range(CHUNKS):
            project(0, c)
    with jax.named_scope("widen"):
        for j in range(1, levs):
            widen(j)
    greeted(0)
    greet(1)

    diag = lax.broadcasted_iota(jnp.int32, (modes, modes), 0) == lax.broadcasted_iota(jnp.int32, (modes, modes), 1)
    helm = jnp.sum(jnp.where(diag, jnp.broadcast_to(helm_own[...], (modes, modes)), 0.0), axis=1, keepdims=True)
    thetas[...] = jnp.broadcast_to(4.0 / (4.0 + helm), (modes, LANE))
    has = {0: tile < tiles - 1, 1: tile > 0}
    for side in range(2):
        @pl.when(jnp.logical_not(has[side]))
        def _(side=side):
            in_buf[:, side] = jnp.zeros_like(in_buf[:, side])

    scale = 2.0 ** 9.7 / (0.5 * 30.0 * levels)

    def halo_first(side, half):
        if side == 0:
            return half * HALF
        return rows - (half + 1) * HALF

    def halo_copy(g, side, half, cols=slice(None)):
        peer = lax.rem(tile + tiles - 1, tiles) if side == 0 else lax.rem(tile + 1, tiles)
        return pltpu.make_async_remote_copy(
            src_ref=out_buf.at[g, side, half, :, cols], dst_ref=in_buf.at[g, side, half, :, cols], send_sem=halo_send.at[g, side, half],
            recv_sem=halo_recv.at[g, side, half], device_id=(peer, lev), device_id_type=MESH)

    sends = {0: tile > 0, 1: tile < tiles - 1}

    def encode_part(g, half, side, cols):
        first = HALO + halo_first(side, half)
        width = cols.stop - cols.start
        out_buf[g, side, half, :, cols] = encode(base[g, first:first + HALF, :, cols].reshape(HALF * SUB, width), scale)

    def send_chunk(c):
        cols = pl.ds(c * chunk, chunk)
        for half in range(2):
            for side in range(2):
                encode_part(0, half, side, slice(c * chunk, (c + 1) * chunk))

                @pl.when(sends[side])
                def _(half=half, side=side):
                    halo_copy(0, side, half, cols).start()

    def send(g):
        with jax.named_scope("send"):
            for half in range(2):
                for side in range(2):
                    encode_part(g, half, side, slice(0, cells))

                    @pl.when(sends[side])
                    def _(half=half, side=side):
                        halo_copy(g, side, half).start()

    with jax.named_scope("other"):
        for c in range(CHUNKS):
            for j in range(1, levs):
                with jax.named_scope("arrive"):
                    swap(j, c).wait_recv()
                project(j, c)
            send_chunk(c)
    greeted(1)
    greet(2)
    for g in range(1, parts):
        send(g)

    lane = lax.broadcasted_iota(jnp.int32, (SUB, LANE), 1)
    first_lane = lane == 0
    last_lane = lane == LANE - 1
    nothing = jnp.zeros((SUB, LANE), f32)

    def beside(tile_row):
        pieces = [tile_row[:, j * LANE:(j + 1) * LANE] for j in range(across)]
        right = [pltpu.roll(piece, 1, 1) for piece in pieces]
        left = [pltpu.roll(piece, LANE - 1, 1) for piece in pieces]
        result = []
        for j in range(across):
            low = jnp.where(first_lane, right[j - 1] if j else nothing, right[j])
            high = jnp.where(last_lane, left[j + 1] if j + 1 < across else nothing, left[j])
            result.append(low + high)
        return jnp.concatenate(result, axis=1)

    def fold(product):
        pieces = [product[:, j * LANE:(j + 1) * LANE] for j in range(across)]
        while len(pieces) > 1:
            pieces = [pieces[i] + pieces[i + 1] if i + 1 < len(pieces) else pieces[i] for i in range(0, len(pieces), 2)]
        return pieces[0]

    inside = jnp.float32(0.5)
    factor = {0: jnp.where(tile > 0, inside, 0.0), 1: jnp.where(tile < tiles - 1, inside, 0.0)}

    places = starts(rows)

    def field(g, k, row):
        if k == 0:
            return base.at[g, row + HALO]
        return powers.at[g, places[k - 1] + row + HALO - k]

    def extend(g, k, ranges):
        totals = {}
        for low, high in ranges:
            for row in range(low, high):
                here = field(g, k - 1, row)[...]
                around = field(g, k - 1, row - 1)[...] + field(g, k - 1, row + 1)[...] + beside(here)
                if row < 0:
                    gain = factor[0]
                elif row >= rows:
                    gain = factor[1]
                else:
                    gain = 0.5
                if k == 1:
                    gain = gain * 0.5
                fresh = gain * around
                if k > 1:
                    fresh = fresh - field(g, k - 2, row)[...]
                field(g, k, row)[...] = fresh
                if 0 <= row < rows:
                    if k == 1:
                        totals[0] = add(totals.get(0), fold(here * here))
                    totals[2 * k - 1] = add(totals.get(2 * k - 1), fold(here * fresh))
                    if k < STEPS:
                        totals[2 * k] = add(totals.get(2 * k), fold(fresh * fresh))
        for slot, value in totals.items():
            sums[g, slot] = sums[g, slot] + value

    def interior(g):
        with jax.named_scope("interior"):
            for k in range(1, STEPS):
                if rows - k > k:
                    extend(g, k, [(k, rows - k)])

    def take(g, half):
        with jax.named_scope("take"):
            for side in range(2):
                @pl.when(has[side])
                def _(side=side):
                    halo_copy(g, side, half).wait_recv()
        with jax.named_scope("decode"):
            for side in range(2):
                if side == 0:
                    first = HALO + rows + half * HALF
                else:
                    first = HALO - (half + 1) * HALF
                base[g, first:first + HALF] = decode(in_buf[g, side, half], scale).reshape(HALF, SUB, cells)

    def outer(g, half):
        with jax.named_scope("outer"):
            old, new = half * HALF, (half + 1) * HALF
            for k in range(1, STEPS + 1):
                extend(g, k, [(k - new, k - old), (rows - k + old, rows - k + new)])

    products = 2 * STEPS
    offset = lane - products * lax.broadcasted_iota(jnp.int32, (SUB, LANE), 0)

    def modes_of(g):
        return pl.ds(pl.multiple_of(g * SUB, SUB), SUB)

    def gram_start(g, stage, table):
        digit, peers = stage_peers[stage]
        grams[g, stage, digit] = table
        for peer in peers:
            pltpu.make_async_remote_copy(
                src_ref=grams.at[g, stage, digit], dst_ref=grams.at[g, stage, digit], send_sem=gram_send.at[g, stage],
                recv_sem=gram_recv.at[g, stage], device_id=(peer, lev), device_id_type=MESH).start()

    def gram_finish(g, stage):
        digit, peers = stage_peers[stage]
        size = groups[stage]
        others = grams.at[g, stage, pl.ds(0, size - 1)]
        pltpu.make_async_remote_copy(
            src_ref=others, dst_ref=others, send_sem=gram_send.at[g, stage],
            recv_sem=gram_recv.at[g, stage], device_id=(peers[0], lev), device_id_type=MESH).wait()
        tables = [grams[g, stage, j] for j in range(size)]
        while len(tables) > 1:
            tables = [tables[i] + tables[i + 1] if i + 1 < len(tables) else tables[i] for i in range(0, len(tables), 2)]
        return tables[0]

    def total(g):
        with jax.named_scope("total"):
            table = jnp.zeros((SUB, LANE), f32)
            for slot in range(products):
                table = jnp.where(offset == slot, jnp.sum(sums[g, slot], axis=1, keepdims=True), table)
            table = jnp.sum(table, axis=0, keepdims=True)
            gram_start(g, 0, table)

    def finish(g):
        with jax.named_scope("gram"):
            for stage in range(len(groups)):
                table = gram_finish(g, stage)
                if stage + 1 < len(groups):
                    gram_start(g, stage + 1, table)
        with jax.named_scope("coef"):
            table = jnp.broadcast_to(table, (SUB, LANE))
            columns = []
            for slot in range(products):
                column = jnp.sum(jnp.where(offset == slot, table, 0.0), axis=1, keepdims=True)
                columns.append(jnp.broadcast_to(column, (SUB, LANE)))
            x, r = coefficients(columns, thetas[modes_of(g)])
        with jax.named_scope("combine"):
            for row in range(rows):
                solved, left = [], []
                for j in range(across):
                    cols = slice(j * LANE, (j + 1) * LANE)
                    x_sum = r_sum = None
                    for k in range(STEPS + 1):
                        value = field(g, k, row)[:, cols]
                        r_sum = add(r_sum, r[k] * value)
                        if k < STEPS:
                            x_sum = add(x_sum, x[k] * value)
                    solved.append(x_sum)
                    left.append(r_sum)
                sol_ref[modes_of(g), row, :] = jnp.concatenate(solved, axis=1)
                res_ref[modes_of(g), row, :] = jnp.concatenate(left, axis=1)

    sums[...] = jnp.zeros_like(sums)

    def each(body):
        def step(index, carry):
            body(index)
            return carry

        lax.fori_loop(0, parts, step, 0)

    def gather(g):
        for half in range(2):
            take(g, half)
            outer(g, half)
        total(g)

    each(interior)
    for r in range(2, len(rounds)):
        greeted(r)
        greet(r + 1)
    each(gather)
    each(finish)

    with jax.named_scope("drain"):
        for j in range(1, levs):
            for c in range(CHUNKS):
                swap(j, c).wait_send()
        for g in range(parts):
            for half in range(2):
                for side in range(2):
                    @pl.when(sends[side])
                    def _(g=g, side=side, half=half):
                        halo_copy(g, side, half).wait_send()


def shards(increments, projection, helmholtz):
    tiles, levs = lax.axis_size("tile"), lax.axis_size("lev")
    own_levels, rows, cells = increments.shape
    modes = projection.shape[0] // levs
    levels = own_levels * levs
    groups = stage_groups(tiles)
    most = max(groups)
    parts = modes // SUB
    vmem = pltpu.VMEM
    dma = pltpu.SemaphoreType.DMA
    scratch = [
        vmem((levs, own_levels * rows, cells), bf16),
        vmem((levs, rows * modes, own_levels * rows), bf16),
        vmem((parts, rows + 2 * HALO, SUB, cells), f32),
        vmem((parts, starts(rows)[-1], SUB, cells), f32),
        vmem((parts, 2, 2, HALF * SUB, cells), bf16),
        vmem((parts, 2, 2, HALF * SUB, cells), bf16),
        vmem((modes, LANE), f32),
        vmem((parts, 2 * STEPS, SUB, LANE), f32),
        vmem((parts, len(groups), most, 1, LANE), f32),
        vmem((levels, levs * modes), bf16),
        vmem((1, modes), f32),
        dma,
        dma((2,)),
        pltpu.SemaphoreType.REGULAR((len(reaches(tiles)) + 1, 2)),
        dma((levs - 1, CHUNKS)),
        dma((levs - 1, CHUNKS)),
        dma((parts, 2, 2)),
        dma((parts, 2, 2)),
        dma((parts, len(groups))),
        dma((parts, len(groups))),
    ]
    shape = pltpu.VMEM((modes, rows, cells), f32)
    return pl.pallas_call(
        functools.partial(kernel, tiles, levs, groups, rows, modes, cells, levels),
        out_shape=(shape, shape),
        in_specs=[pl.BlockSpec(memory_space=pl.ANY)] * 3,
        out_specs=(pl.BlockSpec(memory_space=pltpu.VMEM), pl.BlockSpec(memory_space=pltpu.VMEM)),
        scratch_shapes=scratch,
        compiler_params=pltpu.CompilerParams(collective_id=0, has_side_effects=True, vmem_limit_bytes=52000000),
    )(increments.reshape(own_levels * rows, cells), projection.T, helmholtz.reshape(1, modes))


def solution(mesh):
    in_specs = (P("lev", "tile", None), P(), P("lev"))
    out_specs = (P("lev", "tile", None), P("lev", "tile", None))
    return jax.shard_map(shards, mesh=mesh, in_specs=in_specs, out_specs=out_specs, check_vma=False)
```

```python
import functools

import jax
import jax.numpy as jnp
from jax import lax
from jax.experimental import pallas as pl
from jax.experimental.pallas import tpu as pltpu
from jax.sharding import PartitionSpec as P

STEPS = 8
HALO = STEPS
HALF = HALO // 2
POWER = 13
SUB = 8
LANE = 128
CHUNKS = 4
MESH = pl.DeviceIdType.MESH
f32 = jnp.float32
bf16 = jnp.bfloat16


def stage_groups(count):
    groups = []
    while count > 1:
        size = next(size for size in (16, 4, 2, count) if count % size == 0)
        groups.append(size)
        count //= size
    return groups


def reaches(tiles):
    return [2 ** r for r in range(tiles.bit_length()) if 2 ** r < tiles - 1]


def starts(rows):
    places = [0]
    for k in range(1, STEPS + 1):
        places.append(places[-1] + rows + 2 * (HALO - k))
    return places


def encode(value, scale):
    a = value * scale
    a4 = (a * a) * (a * a)
    return ((a4 * a4) * (a4 * a)).astype(bf16)


def decode(code, scale):
    code = code.astype(f32)
    size = jnp.exp(jnp.log(jnp.maximum(jnp.abs(code), 2.0 ** -126)) * (1.0 / POWER)) * (1.0 / scale)
    return jnp.where(code > 0.0, size, jnp.where(code < 0.0, -size, 0.0))


def add(left, right):
    if left is None:
        return right
    if right is None:
        return left
    return left + right


def coefficients(products, theta):
    count = 2 * STEPS
    moments = list(products[:2])
    for index in range(2, count):
        moments.append(products[index] + products[index] - moments[index % 2])
    half = 0.5 * theta
    one = jnp.ones_like(theta)
    x, r, p = [None] * STEPS, [one], [one]
    r_moments, p_moments = list(moments), list(moments)
    for step in range(STEPS):
        low, high = step, count - 1 - step
        image = {}
        for l in range(low, high):
            if l == 0:
                image[l] = p_moments[0] - theta * p_moments[1]
            else:
                image[l] = p_moments[l] - half * (p_moments[l + 1] + p_moments[l - 1])
        alpha = r_moments[step] / image[step]
        for k in range(step + 1):
            x[k] = add(x[k], alpha * p[k])
        gain = alpha * half
        twice = alpha * theta
        fresh = []
        for k in range(step + 2):
            value = r[k] if k < len(r) else None
            if k < len(p):
                value = value - alpha * p[k] if value is not None else -(alpha * p[k])
            if k == 1:
                value = add(value, twice * p[0])
            elif k > 1:
                value = add(value, gain * p[k - 1])
            if k + 1 < len(p):
                value = value + gain * p[k + 1]
            fresh.append(value)
        r = fresh
        if step == STEPS - 1:
            break
        old = r_moments[step]
        r_moments = [r_moments[l] - alpha * image[l] if l in image else None for l in range(count)]
        beta = (twice if step == 0 else gain) * r_moments[step + 1] / old
        p = [r[k] + beta * p[k] if k < len(p) else r[k] for k in range(step + 2)]
        p_moments = [r_moments[l] + beta * p_moments[l] if l in image else None for l in range(count)]
    return x, r


def write(sol_in, res_in, sol_ref, res_ref, sems):
    copies = [pltpu.make_async_copy(sol_in, sol_ref, sems.at[0]), pltpu.make_async_copy(res_in, res_ref, sems.at[1])]
    for copy in copies:
        copy.start()
    for copy in copies:
        copy.wait()


def kernel(tiles, levs, groups, rows, modes, cells, levels, inc_ref, proj_ref, helm_ref, sol_ref, res_ref,
           x_all, wide, base, powers, out_buf, in_buf, thetas, sums, grams, proj_own, helm_own,
           local_sem, small_sems, known, swap_send, swap_recv, halo_send, halo_recv, gram_send, gram_recv):
    tile = lax.axis_index("tile")
    lev = lax.axis_index("lev")
    part = inc_ref.shape[0]
    across = cells // LANE
    parts = modes // SUB
    barrier = pltpu.get_barrier_semaphore()

    stage_peers = []
    stride = 1
    for size in groups:
        digit = lax.rem(lax.div(tile, stride), size)
        start = tile - digit * stride
        stage_peers.append((digit, [start + lax.rem(digit + j, size) * stride for j in range(1, size)]))
        stride *= size

    count = 0
    for j in range(1, levs):
        pl.semaphore_signal(barrier, 1, device_id=(tile, lax.rem(lev + j, levs)), device_id_type=MESH)
        count += 1
    def toward(distance):
        return [(lax.max(tile - distance, 0), tile >= distance),
                (lax.min(tile + distance, tiles - 1), tile < tiles - distance)]

    for peer, there in toward(1):
        @pl.when(there)
        def _(peer=peer):
            pl.semaphore_signal(barrier, 1, device_id=(peer, lev), device_id_type=MESH)
        count += jnp.where(there, 1, 0)
    local = pltpu.make_async_copy(inc_ref, x_all.at[0], local_sem)
    small = [pltpu.make_async_copy(proj_ref, proj_own, small_sems.at[0]),
             pltpu.make_async_copy(helm_ref, helm_own, small_sems.at[1])]
    for copy in small:
        copy.start()
    local.start()

    chunk = cells // CHUNKS
    with jax.named_scope("barrier"):
        pl.semaphore_wait(barrier, count)

    rounds = reaches(tiles)

    def greet(r):
        if r < len(rounds):
            for way, (peer, there) in enumerate(toward(rounds[r])):
                @pl.when(there)
                def _(way=way, peer=peer):
                    pl.semaphore_signal(known.at[r, way], 1, device_id=(peer, lev), device_id_type=MESH)

    def greeted(r):
        if r < len(rounds):
            for way, (peer, there) in enumerate(toward(rounds[r])):
                @pl.when(there)
                def _(way=way):
                    pl.semaphore_wait(known.at[r, 1 - way], 1)

    greet(0)

    def swap(j, c):
        cols = pl.ds(c * chunk, chunk)
        return pltpu.make_async_remote_copy(
            src_ref=inc_ref.at[:, cols], dst_ref=x_all.at[levs - j, :, cols], send_sem=swap_send.at[j - 1, c],
            recv_sem=swap_recv.at[j - 1, c], device_id=(tile, lax.rem(lev + j, levs)), device_id_type=MESH)

    for c in range(CHUNKS):
        for j in range(1, levs):
            swap(j, c).start()

    for copy in small:
        copy.wait()
    proj = proj_own[...].astype(f32)
    own = proj[:, 0:modes]
    for j in range(1, levs):
        own = jnp.where(lev == j, proj[:, j * modes:(j + 1) * modes], own)
    own_levels = levels // levs
    groups_l = [own[j * own_levels:(j + 1) * own_levels] for j in range(levs)]
    col_e = lax.broadcasted_iota(jnp.int32, (own_levels, part), 1)
    row_e = lax.broadcasted_iota(jnp.int32, (own_levels, part), 0) * rows
    onehot = jnp.where((col_e >= row_e) & (col_e < row_e + rows), 1.0, 0.0).astype(bf16)
    block = rows * SUB
    mask = lax.rem(lax.broadcasted_iota(jnp.int32, (block, part), 1), rows) == lax.div(
        lax.broadcasted_iota(jnp.int32, (block, part), 0), SUB)

    def widen(position):
        chosen = groups_l[position]
        for j in range(1, levs):
            chosen = jnp.where(lev == j, groups_l[(j + position) % levs], chosen)
        repeated = lax.dot_general(
            chosen.astype(bf16), onehot, (((0,), (0,)), ((), ())), preferred_element_type=f32)
        for g in range(parts):
            tall = jnp.concatenate([repeated[g * SUB:(g + 1) * SUB]] * rows, axis=0)
            wide[position, g * block:(g + 1) * block, :] = jnp.where(mask, tall, 0.0).astype(bf16)

    def project(positions, c, first, number, adding=False):
        cols = slice(c * chunk, (c + 1) * chunk)
        got = None
        for position in positions:
            got = add(got, jnp.dot(wide[position, first * block:(first + number) * block], x_all[position, :, cols],
                                   preferred_element_type=f32))
        for g in range(number):
            value = got[g * block:(g + 1) * block].reshape(rows, SUB, chunk)
            if adding:
                value = base[first + g, HALO:HALO + rows, :, cols] + value
            base[first + g, HALO:HALO + rows, :, cols] = value

    with jax.named_scope("widen"):
        widen(0)
    with jax.named_scope("own"):
        local.wait()
        for c in range(CHUNKS):
            project([0], c, 0, 1)
    with jax.named_scope("widen"):
        for j in range(1, levs):
            widen(j)
    greeted(0)
    greet(1)

    diag = lax.broadcasted_iota(jnp.int32, (modes, modes), 0) == lax.broadcasted_iota(jnp.int32, (modes, modes), 1)
    helm = jnp.sum(jnp.where(diag, jnp.broadcast_to(helm_own[...], (modes, modes)), 0.0), axis=1, keepdims=True)
    thetas[...] = jnp.broadcast_to(4.0 / (4.0 + helm), (modes, LANE))
    has = {0: tile < tiles - 1, 1: tile > 0}
    for side in range(2):
        @pl.when(jnp.logical_not(has[side]))
        def _(side=side):
            in_buf[:, side] = jnp.zeros_like(in_buf[:, side])

    scale = 2.0 ** 9.7 / (0.5 * 30.0 * levels)

    def halo_first(side, half):
        if side == 0:
            return half * HALF
        return rows - (half + 1) * HALF

    def halo_copy(g, side, half, cols=slice(None)):
        peer = lax.rem(tile + tiles - 1, tiles) if side == 0 else lax.rem(tile + 1, tiles)
        return pltpu.make_async_remote_copy(
            src_ref=out_buf.at[g, side, half, :, cols], dst_ref=in_buf.at[g, side, half, :, cols], send_sem=halo_send.at[g, side, half],
            recv_sem=halo_recv.at[g, side, half], device_id=(peer, lev), device_id_type=MESH)

    sends = {0: tile > 0, 1: tile < tiles - 1}

    def encode_part(g, half, side, cols):
        first = HALO + halo_first(side, half)
        width = cols.stop - cols.start
        out_buf[g, side, half, :, cols] = encode(base[g, first:first + HALF, :, cols].reshape(HALF * SUB, width), scale)

    def send_chunk(g, c):
        cols = pl.ds(c * chunk, chunk)
        for half in range(2):
            for side in range(2):
                encode_part(g, half, side, slice(c * chunk, (c + 1) * chunk))

                @pl.when(sends[side])
                def _(half=half, side=side):
                    halo_copy(g, side, half, cols).start()

    def send(g):
        with jax.named_scope("send"):
            for half in range(2):
                for side in range(2):
                    encode_part(g, half, side, slice(0, cells))

                    @pl.when(sends[side])
                    def _(half=half, side=side):
                        halo_copy(g, side, half).start()

    with jax.named_scope("other"):
        for c in range(CHUNKS):
            with jax.named_scope("arrive"):
                for j in range(1, levs):
                    swap(j, c).wait_recv()
            project(range(1, levs), c, 0, 1, True)
            send_chunk(0, c)
    greeted(1)
    greet(2)
    with jax.named_scope("rest"):
        for c in range(CHUNKS):
            for g in range(1, parts, 2):
                project(range(levs), c, g, min(2, parts - g))
            if parts > 1:
                send_chunk(1, c)
    for g in range(2, parts):
        send(g)

    lane = lax.broadcasted_iota(jnp.int32, (SUB, LANE), 1)
    first_lane = lane == 0
    last_lane = lane == LANE - 1
    nothing = jnp.zeros((SUB, LANE), f32)

    def beside(tile_row):
        pieces = [tile_row[:, j * LANE:(j + 1) * LANE] for j in range(across)]
        right = [pltpu.roll(piece, 1, 1) for piece in pieces]
        left = [pltpu.roll(piece, LANE - 1, 1) for piece in pieces]
        result = []
        for j in range(across):
            low = jnp.where(first_lane, right[j - 1] if j else nothing, right[j])
            high = jnp.where(last_lane, left[j + 1] if j + 1 < across else nothing, left[j])
            result.append(low + high)
        return jnp.concatenate(result, axis=1)

    def fold(product):
        pieces = [product[:, j * LANE:(j + 1) * LANE] for j in range(across)]
        while len(pieces) > 1:
            pieces = [pieces[i] + pieces[i + 1] if i + 1 < len(pieces) else pieces[i] for i in range(0, len(pieces), 2)]
        return pieces[0]

    inside = jnp.float32(0.5)
    factor = {0: jnp.where(tile > 0, inside, 0.0), 1: jnp.where(tile < tiles - 1, inside, 0.0)}

    places = starts(rows)

    def field(g, k, row):
        if k == 0:
            return base.at[g, row + HALO]
        return powers.at[g, places[k - 1] + row + HALO - k]

    def extend(g, k, ranges):
        totals = {}
        for low, high in ranges:
            for row in range(low, high):
                here = field(g, k - 1, row)[...]
                around = field(g, k - 1, row - 1)[...] + field(g, k - 1, row + 1)[...] + beside(here)
                if row < 0:
                    gain = factor[0]
                elif row >= rows:
                    gain = factor[1]
                else:
                    gain = 0.5
                if k == 1:
                    gain = gain * 0.5
                fresh = gain * around
                if k > 1:
                    fresh = fresh - field(g, k - 2, row)[...]
                field(g, k, row)[...] = fresh
                if 0 <= row < rows:
                    if k == 1:
                        totals[0] = add(totals.get(0), fold(here * here))
                    totals[2 * k - 1] = add(totals.get(2 * k - 1), fold(here * fresh))
                    if k < STEPS:
                        totals[2 * k] = add(totals.get(2 * k), fold(fresh * fresh))
        for slot, value in totals.items():
            sums[g, slot] = sums[g, slot] + value

    def interior(g):
        with jax.named_scope("interior"):
            for k in range(1, STEPS):
                if rows - k > k:
                    extend(g, k, [(k, rows - k)])

    def take(g, half, side):
        with jax.named_scope("take"):
            @pl.when(has[side])
            def _():
                halo_copy(g, side, half).wait_recv()
        with jax.named_scope("decode"):
            if side == 0:
                first = HALO + rows + half * HALF
            else:
                first = HALO - (half + 1) * HALF
            base[g, first:first + HALF] = decode(in_buf[g, side, half], scale).reshape(HALF, SUB, cells)

    def outer(g, half, sides):
        with jax.named_scope("outer"):
            old, new = half * HALF, (half + 1) * HALF
            for k in range(1, STEPS + 1):
                ranges = {0: (rows - k + old, rows - k + new), 1: (k - new, k - old)}
                extend(g, k, [ranges[side] for side in sides])

    products = 2 * STEPS
    offset = lane - products * lax.broadcasted_iota(jnp.int32, (SUB, LANE), 0)

    def modes_of(g):
        return pl.ds(pl.multiple_of(g * SUB, SUB), SUB)

    def gram_start(g, stage, table):
        digit, peers = stage_peers[stage]
        grams[g, stage, digit] = table
        for peer in peers:
            pltpu.make_async_remote_copy(
                src_ref=grams.at[g, stage, digit], dst_ref=grams.at[g, stage, digit], send_sem=gram_send.at[g, stage],
                recv_sem=gram_recv.at[g, stage], device_id=(peer, lev), device_id_type=MESH).start()

    def gram_finish(g, stage):
        digit, peers = stage_peers[stage]
        size = groups[stage]
        others = grams.at[g, stage, pl.ds(0, size - 1)]
        pltpu.make_async_remote_copy(
            src_ref=others, dst_ref=others, send_sem=gram_send.at[g, stage],
            recv_sem=gram_recv.at[g, stage], device_id=(peers[0], lev), device_id_type=MESH).wait()
        tables = [grams[g, stage, j] for j in range(size)]
        while len(tables) > 1:
            tables = [tables[i] + tables[i + 1] if i + 1 < len(tables) else tables[i] for i in range(0, len(tables), 2)]
        return tables[0]

    def total(g):
        with jax.named_scope("total"):
            table = jnp.zeros((SUB, LANE), f32)
            for slot in range(products):
                table = jnp.where(offset == slot, jnp.sum(sums[g, slot], axis=1, keepdims=True), table)
            table = jnp.sum(table, axis=0, keepdims=True)
            gram_start(g, 0, table)

    def finish(g):
        with jax.named_scope("gram"):
            for stage in range(len(groups)):
                table = gram_finish(g, stage)
                if stage + 1 < len(groups):
                    gram_start(g, stage + 1, table)
        with jax.named_scope("coef"):
            table = jnp.broadcast_to(table, (SUB, LANE))
            columns = []
            for slot in range(products):
                column = jnp.sum(jnp.where(offset == slot, table, 0.0), axis=1, keepdims=True)
                columns.append(jnp.broadcast_to(column, (SUB, LANE)))
            x, r = coefficients(columns, thetas[modes_of(g)])
        with jax.named_scope("combine"):
            for row in range(rows):
                solved, left = [], []
                for j in range(across):
                    cols = slice(j * LANE, (j + 1) * LANE)
                    x_sum = r_sum = None
                    for k in range(STEPS + 1):
                        value = field(g, k, row)[:, cols]
                        r_sum = add(r_sum, r[k] * value)
                        if k < STEPS:
                            x_sum = add(x_sum, x[k] * value)
                    solved.append(x_sum)
                    left.append(r_sum)
                sol_ref[modes_of(g), row, :] = jnp.concatenate(solved, axis=1)
                res_ref[modes_of(g), row, :] = jnp.concatenate(left, axis=1)

    sums[...] = jnp.zeros_like(sums)

    def each(body):
        def step(index, carry):
            body(index)
            return carry

        lax.fori_loop(0, parts, step, 0)

    def gather(g):
        for half in range(2):
            for side in range(2):
                take(g, half, side)
            outer(g, half, (1, 0))
        total(g)

    each(interior)
    for r in range(2, len(rounds)):
        greeted(r)
        greet(r + 1)
    each(gather)
    each(finish)

    with jax.named_scope("drain"):
        for j in range(1, levs):
            for c in range(CHUNKS):
                swap(j, c).wait_send()
        for g in range(parts):
            for half in range(2):
                for side in range(2):
                    @pl.when(sends[side])
                    def _(g=g, side=side, half=half):
                        halo_copy(g, side, half).wait_send()


def shards(increments, projection, helmholtz):
    tiles, levs = lax.axis_size("tile"), lax.axis_size("lev")
    own_levels, rows, cells = increments.shape
    modes = projection.shape[0] // levs
    levels = own_levels * levs
    groups = stage_groups(tiles)
    most = max(groups)
    parts = modes // SUB
    vmem = pltpu.VMEM
    dma = pltpu.SemaphoreType.DMA
    scratch = [
        vmem((levs, own_levels * rows, cells), bf16),
        vmem((levs, rows * modes, own_levels * rows), bf16),
        vmem((parts, rows + 2 * HALO, SUB, cells), f32),
        vmem((parts, starts(rows)[-1], SUB, cells), f32),
        vmem((parts, 2, 2, HALF * SUB, cells), bf16),
        vmem((parts, 2, 2, HALF * SUB, cells), bf16),
        vmem((modes, LANE), f32),
        vmem((parts, 2 * STEPS, SUB, LANE), f32),
        vmem((parts, len(groups), most, 1, LANE), f32),
        vmem((levels, levs * modes), bf16),
        vmem((1, modes), f32),
        dma,
        dma((2,)),
        pltpu.SemaphoreType.REGULAR((len(reaches(tiles)) + 1, 2)),
        dma((levs - 1, CHUNKS)),
        dma((levs - 1, CHUNKS)),
        dma((parts, 2, 2)),
        dma((parts, 2, 2)),
        dma((parts, len(groups))),
        dma((parts, len(groups))),
    ]
    shape = pltpu.VMEM((modes, rows, cells), f32)
    kept = pl.pallas_call(
        functools.partial(kernel, tiles, levs, groups, rows, modes, cells, levels),
        out_shape=(shape, shape),
        in_specs=[pl.BlockSpec(memory_space=pl.ANY)] * 3,
        out_specs=(pl.BlockSpec(memory_space=pltpu.VMEM), pl.BlockSpec(memory_space=pltpu.VMEM)),
        scratch_shapes=scratch,
        compiler_params=pltpu.CompilerParams(collective_id=0, has_side_effects=True, vmem_limit_bytes=52000000),
    )(increments.reshape(own_levels * rows, cells), projection.T, helmholtz.reshape(1, modes))
    outside = pl.BlockSpec(memory_space=pl.ANY)
    inside = pl.BlockSpec(memory_space=vmem)
    shape = jax.ShapeDtypeStruct((modes, rows, cells), f32)
    return pl.pallas_call(
        write, out_shape=(shape, shape), in_specs=[inside] * 2, out_specs=(outside, outside),
        scratch_shapes=[dma((2,))], compiler_params=pltpu.CompilerParams(vmem_limit_bytes=1000000),
    )(*kept)


def solution(mesh):
    in_specs = (P("lev", "tile", None), P(), P("lev"))
    out_specs = (P("lev", "tile", None), P("lev", "tile", None))
    return jax.shard_map(shards, mesh=mesh, in_specs=in_specs, out_specs=out_specs, check_vma=False)
```

```python
import functools

import jax
import jax.numpy as jnp
from jax import lax
from jax.experimental import pallas as pl
from jax.experimental.pallas import tpu as pltpu
from jax.sharding import PartitionSpec as P

STEPS = 8
HALO = STEPS
HALF = HALO // 2
POWER = 13
SUB = 8
LANE = 128
CHUNKS = 8
WIDER = 2
MESH = pl.DeviceIdType.MESH
f32 = jnp.float32
bf16 = jnp.bfloat16


def stage_groups(count):
    groups = []
    while count > 1:
        size = next(size for size in (16, 4, 2, count) if count % size == 0)
        groups.append(size)
        count //= size
    return groups


def reaches(tiles):
    return [2 ** r for r in range(tiles.bit_length()) if 2 ** r < tiles - 1]


def starts(rows):
    places = [0]
    for k in range(1, STEPS + 1):
        places.append(places[-1] + rows + 2 * (HALO - k))
    return places


def encode(value, scale):
    a = value * scale
    a4 = (a * a) * (a * a)
    return ((a4 * a4) * (a4 * a)).astype(bf16)


def decode(code, scale):
    code = code.astype(f32)
    size = jnp.exp(jnp.log(jnp.maximum(jnp.abs(code), 2.0 ** -126)) * (1.0 / POWER)) * (1.0 / scale)
    return jnp.where(code > 0.0, size, jnp.where(code < 0.0, -size, 0.0))


def add(left, right):
    if left is None:
        return right
    if right is None:
        return left
    return left + right


def coefficients(products, theta):
    count = 2 * STEPS
    moments = list(products[:2])
    for index in range(2, count):
        moments.append(products[index] + products[index] - moments[index % 2])
    half = 0.5 * theta
    one = jnp.ones_like(theta)
    x, r, p = [None] * STEPS, [one], [one]
    r_moments, p_moments = list(moments), list(moments)
    for step in range(STEPS):
        low, high = step, count - 1 - step
        image = {}
        for l in range(low, high):
            if l == 0:
                image[l] = p_moments[0] - theta * p_moments[1]
            else:
                image[l] = p_moments[l] - half * (p_moments[l + 1] + p_moments[l - 1])
        alpha = r_moments[step] / image[step]
        for k in range(step + 1):
            x[k] = add(x[k], alpha * p[k])
        gain = alpha * half
        twice = alpha * theta
        fresh = []
        for k in range(step + 2):
            value = r[k] if k < len(r) else None
            if k < len(p):
                value = value - alpha * p[k] if value is not None else -(alpha * p[k])
            if k == 1:
                value = add(value, twice * p[0])
            elif k > 1:
                value = add(value, gain * p[k - 1])
            if k + 1 < len(p):
                value = value + gain * p[k + 1]
            fresh.append(value)
        r = fresh
        if step == STEPS - 1:
            break
        old = r_moments[step]
        r_moments = [r_moments[l] - alpha * image[l] if l in image else None for l in range(count)]
        beta = (twice if step == 0 else gain) * r_moments[step + 1] / old
        p = [r[k] + beta * p[k] if k < len(p) else r[k] for k in range(step + 2)]
        p_moments = [r_moments[l] + beta * p_moments[l] if l in image else None for l in range(count)]
    return x, r


def combine(first, powers, x, r, solved, left):
    rows, cells = solved.shape[1:]
    places = starts(rows)
    for row in range(rows):
        for j in range(cells // LANE):
            cols = slice(j * LANE, (j + 1) * LANE)
            x_sum = r_sum = None
            for k in range(STEPS + 1):
                if k == 0:
                    value = first[row + HALO, :, cols]
                else:
                    value = powers[places[k - 1] + row + HALO - k, :, cols]
                r_sum = add(r_sum, r[k] * value)
                if k < STEPS:
                    x_sum = add(x_sum, x[k] * value)
            solved[:, row, cols] = x_sum
            left[:, row, cols] = r_sum


def write(parts, sol_in, res_in, base, tail, last, sol_ref, res_ref, ready, sems):
    done = (parts - 1) * SUB
    copies = []

    def put(src, dst):
        copy = pltpu.make_async_copy(src, dst, sems.at[len(copies)])
        copy.start()
        copies.append(copy)

    if done:
        put(sol_in, sol_ref.at[pl.ds(0, done)])
        put(res_in, res_ref.at[pl.ds(0, done)])
    coefs = [last[k] for k in range(2 * STEPS + 1)]
    combine(base.at[parts - 1], tail, coefs[:STEPS], coefs[STEPS:], ready.at[0], ready.at[1])
    put(ready.at[0], sol_ref.at[pl.ds(done, SUB)])
    put(ready.at[1], res_ref.at[pl.ds(done, SUB)])
    for copy in copies:
        copy.wait()


def kernel(tiles, levs, groups, rows, modes, cells, levels, inc_ref, proj_ref, helm_ref, sol_ref, res_ref, base, tail, last,
           x_all, wide, powers, out_buf, in_buf, thetas, sums, grams, proj_own, helm_own,
           local_sem, small_sems, known, swap_send, swap_recv, halo_send, halo_recv, gram_send, gram_recv):
    tile = lax.axis_index("tile")
    lev = lax.axis_index("lev")
    part = inc_ref.shape[0]
    across = cells // LANE
    parts = modes // SUB
    barrier = pltpu.get_barrier_semaphore()

    stage_peers = []
    stride = 1
    for size in groups:
        digit = lax.rem(lax.div(tile, stride), size)
        start = tile - digit * stride
        stage_peers.append((digit, [start + lax.rem(digit + j, size) * stride for j in range(1, size)]))
        stride *= size

    count = 0
    for j in range(1, levs):
        pl.semaphore_signal(barrier, 1, device_id=(tile, lax.rem(lev + j, levs)), device_id_type=MESH)
        count += 1
    def toward(distance):
        return [(lax.max(tile - distance, 0), tile >= distance),
                (lax.min(tile + distance, tiles - 1), tile < tiles - distance)]

    for peer, there in toward(1):
        @pl.when(there)
        def _(peer=peer):
            pl.semaphore_signal(barrier, 1, device_id=(peer, lev), device_id_type=MESH)
        count += jnp.where(there, 1, 0)
    local = pltpu.make_async_copy(inc_ref, x_all.at[0], local_sem)
    small = [pltpu.make_async_copy(proj_ref, proj_own, small_sems.at[0]),
             pltpu.make_async_copy(helm_ref, helm_own, small_sems.at[1])]
    for copy in small:
        copy.start()
    local.start()

    chunk = cells // CHUNKS
    with jax.named_scope("barrier"):
        pl.semaphore_wait(barrier, count)

    rounds = reaches(tiles)

    def greet(r):
        if r < len(rounds):
            for way, (peer, there) in enumerate(toward(rounds[r])):
                @pl.when(there)
                def _(way=way, peer=peer):
                    pl.semaphore_signal(known.at[r, way], 1, device_id=(peer, lev), device_id_type=MESH)

    def greeted(r):
        if r < len(rounds):
            for way, (peer, there) in enumerate(toward(rounds[r])):
                @pl.when(there)
                def _(way=way):
                    pl.semaphore_wait(known.at[r, 1 - way], 1)

    greet(0)

    def swap(j, c):
        cols = pl.ds(c * chunk, chunk)
        return pltpu.make_async_remote_copy(
            src_ref=inc_ref.at[:, cols], dst_ref=x_all.at[levs - j, :, cols], send_sem=swap_send.at[j - 1, c],
            recv_sem=swap_recv.at[j - 1, c], device_id=(tile, lax.rem(lev + j, levs)), device_id_type=MESH)

    for c in range(CHUNKS):
        for j in range(1, levs):
            swap(j, c).start()

    for copy in small:
        copy.wait()
    proj = proj_own[...].astype(f32)
    own = proj[:, 0:modes]
    for j in range(1, levs):
        own = jnp.where(lev == j, proj[:, j * modes:(j + 1) * modes], own)
    own_levels = levels // levs
    groups_l = [own[j * own_levels:(j + 1) * own_levels] for j in range(levs)]
    col_e = lax.broadcasted_iota(jnp.int32, (own_levels, part), 1)
    row_e = lax.broadcasted_iota(jnp.int32, (own_levels, part), 0) * rows
    onehot = jnp.where((col_e >= row_e) & (col_e < row_e + rows), 1.0, 0.0).astype(bf16)
    block = rows * SUB
    mask = lax.rem(lax.broadcasted_iota(jnp.int32, (block, part), 1), rows) == lax.div(
        lax.broadcasted_iota(jnp.int32, (block, part), 0), SUB)

    def widen(position):
        chosen = groups_l[position]
        for j in range(1, levs):
            chosen = jnp.where(lev == j, groups_l[(j + position) % levs], chosen)
        repeated = lax.dot_general(
            chosen.astype(bf16), onehot, (((0,), (0,)), ((), ())), preferred_element_type=f32)
        for g in range(parts):
            tall = jnp.concatenate([repeated[g * SUB:(g + 1) * SUB]] * rows, axis=0)
            wide[position, g * block:(g + 1) * block, :] = jnp.where(mask, tall, 0.0).astype(bf16)

    def project(positions, c, first, number, adding=False, wide_by=1):
        cols = slice(c * chunk, (c + wide_by) * chunk)
        got = None
        for position in positions:
            got = add(got, jnp.dot(wide[position, first * block:(first + number) * block], x_all[position, :, cols],
                                   preferred_element_type=f32))
        for g in range(number):
            value = got[g * block:(g + 1) * block].reshape(rows, SUB, wide_by * chunk)
            if adding:
                value = base[first + g, HALO:HALO + rows, :, cols] + value
            base[first + g, HALO:HALO + rows, :, cols] = value

    with jax.named_scope("widen"):
        widen(0)
    with jax.named_scope("own"):
        local.wait()
        for c in range(0, CHUNKS, WIDER):
            project([0], c, 0, 1, wide_by=WIDER)
    with jax.named_scope("widen"):
        for j in range(1, levs):
            widen(j)
    greeted(0)
    greet(1)

    diag = lax.broadcasted_iota(jnp.int32, (modes, modes), 0) == lax.broadcasted_iota(jnp.int32, (modes, modes), 1)
    helm = jnp.sum(jnp.where(diag, jnp.broadcast_to(helm_own[...], (modes, modes)), 0.0), axis=1, keepdims=True)
    thetas[...] = jnp.broadcast_to(4.0 / (4.0 + helm), (modes, LANE))
    has = {0: tile < tiles - 1, 1: tile > 0}
    for side in range(2):
        @pl.when(jnp.logical_not(has[side]))
        def _(side=side):
            in_buf[:, side] = jnp.zeros_like(in_buf[:, side])

    scale = 2.0 ** 9.7 / (0.5 * 30.0 * levels)

    def halo_first(side, half):
        if side == 0:
            return half * HALF
        return rows - (half + 1) * HALF

    def halo_copy(g, side, half, cols=slice(None)):
        peer = lax.rem(tile + tiles - 1, tiles) if side == 0 else lax.rem(tile + 1, tiles)
        return pltpu.make_async_remote_copy(
            src_ref=out_buf.at[g, side, half, :, cols], dst_ref=in_buf.at[g, side, half, :, cols], send_sem=halo_send.at[g, side, half],
            recv_sem=halo_recv.at[g, side, half], device_id=(peer, lev), device_id_type=MESH)

    sends = {0: tile > 0, 1: tile < tiles - 1}

    def encode_part(g, half, side, cols):
        first = HALO + halo_first(side, half)
        width = cols.stop - cols.start
        out_buf[g, side, half, :, cols] = encode(base[g, first:first + HALF, :, cols].reshape(HALF * SUB, width), scale)

    def send_chunk(g, c, wide_by=1):
        cols = pl.ds(c * chunk, wide_by * chunk)
        for half in range(2):
            for side in range(2):
                encode_part(g, half, side, slice(c * chunk, (c + wide_by) * chunk))

                @pl.when(sends[side])
                def _(half=half, side=side):
                    halo_copy(g, side, half, cols).start()

    def send(g):
        with jax.named_scope("send"):
            for half in range(2):
                for side in range(2):
                    encode_part(g, half, side, slice(0, cells))

                    @pl.when(sends[side])
                    def _(half=half, side=side):
                        halo_copy(g, side, half).start()

    with jax.named_scope("other"):
        for c in range(CHUNKS):
            with jax.named_scope("arrive"):
                for j in range(1, levs):
                    swap(j, c).wait_recv()
            project(range(1, levs), c, 0, 1, True)
            send_chunk(0, c)
    greeted(1)
    greet(2)
    with jax.named_scope("rest"):
        for c in range(0, CHUNKS, WIDER):
            for g in range(1, parts, 2):
                project(range(levs), c, g, min(2, parts - g), wide_by=WIDER)
            if parts > 1:
                send_chunk(1, c, WIDER)
    for g in range(2, parts):
        send(g)

    lane = lax.broadcasted_iota(jnp.int32, (SUB, LANE), 1)
    first_lane = lane == 0
    last_lane = lane == LANE - 1
    nothing = jnp.zeros((SUB, LANE), f32)

    def beside(tile_row):
        pieces = [tile_row[:, j * LANE:(j + 1) * LANE] for j in range(across)]
        right = [pltpu.roll(piece, 1, 1) for piece in pieces]
        left = [pltpu.roll(piece, LANE - 1, 1) for piece in pieces]
        result = []
        for j in range(across):
            low = jnp.where(first_lane, right[j - 1] if j else nothing, right[j])
            high = jnp.where(last_lane, left[j + 1] if j + 1 < across else nothing, left[j])
            result.append(low + high)
        return jnp.concatenate(result, axis=1)

    def fold(product):
        pieces = [product[:, j * LANE:(j + 1) * LANE] for j in range(across)]
        while len(pieces) > 1:
            pieces = [pieces[i] + pieces[i + 1] if i + 1 < len(pieces) else pieces[i] for i in range(0, len(pieces), 2)]
        return pieces[0]

    inside = jnp.float32(0.5)
    factor = {0: jnp.where(tile > 0, inside, 0.0), 1: jnp.where(tile < tiles - 1, inside, 0.0)}

    places = starts(rows)

    def field(g, k, row):
        if k == 0:
            return base.at[g, row + HALO]
        at = places[k - 1] + row + HALO - k
        if isinstance(g, int) and g == parts - 1:
            return tail.at[at]
        return powers.at[g, at]

    def extend(g, k, ranges):
        totals = {}
        for low, high in ranges:
            for row in range(low, high):
                here = field(g, k - 1, row)[...]
                around = field(g, k - 1, row - 1)[...] + field(g, k - 1, row + 1)[...] + beside(here)
                if row < 0:
                    gain = factor[0]
                elif row >= rows:
                    gain = factor[1]
                else:
                    gain = 0.5
                if k == 1:
                    gain = gain * 0.5
                fresh = gain * around
                if k > 1:
                    fresh = fresh - field(g, k - 2, row)[...]
                field(g, k, row)[...] = fresh
                if 0 <= row < rows:
                    if k == 1:
                        totals[0] = add(totals.get(0), fold(here * here))
                    totals[2 * k - 1] = add(totals.get(2 * k - 1), fold(here * fresh))
                    if k < STEPS:
                        totals[2 * k] = add(totals.get(2 * k), fold(fresh * fresh))
        for slot, value in totals.items():
            sums[g, slot] = sums[g, slot] + value

    def interior(g):
        with jax.named_scope("interior"):
            for k in range(1, STEPS):
                if rows - k > k:
                    extend(g, k, [(k, rows - k)])

    def take(g, half, side):
        with jax.named_scope("take"):
            @pl.when(has[side])
            def _():
                halo_copy(g, side, half).wait_recv()
        with jax.named_scope("decode"):
            if side == 0:
                first = HALO + rows + half * HALF
            else:
                first = HALO - (half + 1) * HALF
            base[g, first:first + HALF] = decode(in_buf[g, side, half], scale).reshape(HALF, SUB, cells)

    def outer(g, half, sides):
        with jax.named_scope("outer"):
            old, new = half * HALF, (half + 1) * HALF
            for k in range(1, STEPS + 1):
                ranges = {0: (rows - k + old, rows - k + new), 1: (k - new, k - old)}
                extend(g, k, [ranges[side] for side in sides])

    products = 2 * STEPS
    offset = lane - products * lax.broadcasted_iota(jnp.int32, (SUB, LANE), 0)

    def modes_of(g):
        return pl.ds(pl.multiple_of(g * SUB, SUB), SUB)

    def gram_start(g, stage, table):
        digit, peers = stage_peers[stage]
        grams[g, stage, digit] = table
        for peer in peers:
            pltpu.make_async_remote_copy(
                src_ref=grams.at[g, stage, digit], dst_ref=grams.at[g, stage, digit], send_sem=gram_send.at[g, stage],
                recv_sem=gram_recv.at[g, stage], device_id=(peer, lev), device_id_type=MESH).start()

    def gram_finish(g, stage):
        digit, peers = stage_peers[stage]
        size = groups[stage]
        others = grams.at[g, stage, pl.ds(0, size - 1)]
        pltpu.make_async_remote_copy(
            src_ref=others, dst_ref=others, send_sem=gram_send.at[g, stage],
            recv_sem=gram_recv.at[g, stage], device_id=(peers[0], lev), device_id_type=MESH).wait()
        tables = [grams[g, stage, j] for j in range(size)]
        while len(tables) > 1:
            tables = [tables[i] + tables[i + 1] if i + 1 < len(tables) else tables[i] for i in range(0, len(tables), 2)]
        return tables[0]

    def total(g):
        with jax.named_scope("total"):
            table = jnp.zeros((SUB, LANE), f32)
            for slot in range(products):
                table = jnp.where(offset == slot, jnp.sum(sums[g, slot], axis=1, keepdims=True), table)
            table = jnp.sum(table, axis=0, keepdims=True)
            gram_start(g, 0, table)

    def solve(g):
        with jax.named_scope("gram"):
            for stage in range(len(groups)):
                table = gram_finish(g, stage)
                if stage + 1 < len(groups):
                    gram_start(g, stage + 1, table)
        with jax.named_scope("coef"):
            table = jnp.broadcast_to(table, (SUB, LANE))
            columns = []
            for slot in range(products):
                column = jnp.sum(jnp.where(offset == slot, table, 0.0), axis=1, keepdims=True)
                columns.append(jnp.broadcast_to(column, (SUB, LANE)))
            return coefficients(columns, thetas[modes_of(g)])

    def finish(g):
        x, r = solve(g)
        with jax.named_scope("combine"):
            combine(base.at[g], powers.at[g], x, r, sol_ref.at[modes_of(g)], res_ref.at[modes_of(g)])

    sums[...] = jnp.zeros_like(sums)

    def each(body, number=parts, start=0):
        def step(index, carry):
            body(index)
            return carry

        lax.fori_loop(start, number, step, 0)

    def gather(g):
        for half in range(2):
            for side in range(2):
                take(g, half, side)
            outer(g, half, (1, 0))
        total(g)

    each(interior, parts - 1)
    interior(parts - 1)
    for r in range(2, len(rounds)):
        greeted(r)
        greet(r + 1)
    each(gather, parts - 1)
    gather(parts - 1)
    each(finish, parts - 1)
    x, r = solve(parts - 1)
    for k, value in enumerate(x + r):
        last[k] = value

    with jax.named_scope("drain"):
        for j in range(1, levs):
            for c in range(CHUNKS):
                swap(j, c).wait_send()
        for g in range(parts):
            for half in range(2):
                for side in range(2):
                    @pl.when(sends[side])
                    def _(g=g, side=side, half=half):
                        halo_copy(g, side, half).wait_send()


def shards(increments, projection, helmholtz):
    tiles, levs = lax.axis_size("tile"), lax.axis_size("lev")
    own_levels, rows, cells = increments.shape
    modes = projection.shape[0] // levs
    levels = own_levels * levs
    groups = stage_groups(tiles)
    most = max(groups)
    parts = modes // SUB
    vmem = pltpu.VMEM
    dma = pltpu.SemaphoreType.DMA
    scratch = [
        vmem((levs, own_levels * rows, cells), bf16),
        vmem((levs, rows * modes, own_levels * rows), bf16),
        vmem((max(parts - 1, 1), starts(rows)[-1], SUB, cells), f32),
        vmem((parts, 2, 2, HALF * SUB, cells), bf16),
        vmem((parts, 2, 2, HALF * SUB, cells), bf16),
        vmem((modes, LANE), f32),
        vmem((parts, 2 * STEPS, SUB, LANE), f32),
        vmem((parts, len(groups), most, 1, LANE), f32),
        vmem((levels, levs * modes), bf16),
        vmem((1, modes), f32),
        dma,
        dma((2,)),
        pltpu.SemaphoreType.REGULAR((len(reaches(tiles)) + 1, 2)),
        dma((levs - 1, CHUNKS)),
        dma((levs - 1, CHUNKS)),
        dma((parts, 2, 2)),
        dma((parts, 2, 2)),
        dma((parts, len(groups))),
        dma((parts, len(groups))),
    ]
    shape = vmem((max(parts - 1, 1) * SUB, rows, cells), f32)
    held = (shape, shape, vmem((parts, rows + 2 * HALO, SUB, cells), f32),
            vmem((starts(rows)[-1], SUB, cells), f32), vmem((2 * STEPS + 1, SUB, LANE), f32))
    inside = pl.BlockSpec(memory_space=vmem)
    outside = pl.BlockSpec(memory_space=pl.ANY)
    kept = pl.pallas_call(
        functools.partial(kernel, tiles, levs, groups, rows, modes, cells, levels),
        out_shape=held,
        in_specs=[outside] * 3,
        out_specs=(inside,) * len(held),
        scratch_shapes=scratch,
        compiler_params=pltpu.CompilerParams(collective_id=0, has_side_effects=True, vmem_limit_bytes=50000000),
    )(increments.reshape(own_levels * rows, cells), projection.T, helmholtz.reshape(1, modes))
    shape = jax.ShapeDtypeStruct((modes, rows, cells), f32)
    return pl.pallas_call(
        functools.partial(write, parts),
        out_shape=(shape, shape),
        in_specs=[inside] * len(held),
        out_specs=(outside, outside),
        scratch_shapes=[vmem((2, SUB, rows, cells), f32), dma((4,))],
        compiler_params=pltpu.CompilerParams(vmem_limit_bytes=3000000),
    )(*kept)


def solution(mesh):
    in_specs = (P("lev", "tile", None), P(), P("lev"))
    out_specs = (P("lev", "tile", None), P("lev", "tile", None))
    return jax.shard_map(shards, mesh=mesh, in_specs=in_specs, out_specs=out_specs, check_vma=False)
```
